128 devices in a mesh: grp: 4 (over x), dom: 32 (over z, y, core).
Axes of the slice: x: 4, y: 4, z: 4, core: 2. Of those that a mesh axis runs over, the one named last changes fastest.
Arguments:
- displacement: float32 [4, 3, 64, 96, 128], P('grp', None, 'dom'), may hold values from -3 to 3
- velocity: float32 [4, 3, 64, 96, 128], P('grp', None, 'dom'), may hold values from -6 to 6
- external: float32 [4, 3, 64, 96, 128], P('grp', None, 'dom'), may hold values from -6 to 6
- mass: float32 [4, 64, 96, 128], P('grp', 'dom'), may hold values from 1 to 3
- elem_scale: float32 [4, 64, 96, 128], P('grp', 'dom'), may hold values from 0.05 to 0.5
- stiffness: float32 [4, 24, 24], P('grp'), as said below
- substeps: int32 [4], P('grp'), may hold values from 1 to 8
- own_nodes: int32 [4, 512], P('grp', 'dom'), may hold values from 0 to 24575, as said below
- peer_nodes: int32 [4, 512], P('grp', 'dom'), may hold values from 0 to 24575, as said below
- normals: float32 [4, 3, 512], P('grp', None, 'dom'), may hold values from -4 to 4
- schur_inverse: float32 [2048, 2048], P(('grp', 'dom')), as said below
Outputs:
- new_displacement: float32 [4, 3, 64, 96, 128], P('grp', None, 'dom')
- new_velocity: float32 [4, 3, 64, 96, 128], P('grp', None, 'dom')
The draws below stay inside these ranges and needn't reach their ends.
Inputs may be any that keep to these rules, and one draw needn't show every extreme that they name: `own_nodes`: the 16 entries of one device's block are distinct. `peer_nodes`: the 16 entries of one device's block are distinct. `schur_inverse`: symmetric. `stiffness`: symmetric positive definite.
All inputs are finite; a program needn't handle non-finite values.
Results may differ from the reference program's by a relative error of at most 0.0001.
Values sent between devices are 32-bit elements; how exact they have to be, the bound alone decides.
No kernel may reach another device: no remote copies, remote signals or barrier semaphores. Data moves between devices by JAX's collectives and lax.ppermute only.
A program may use at most 64 MiB of HBM per device.

```python
import math
import jax
import jax.numpy as jnp
from jax import lax

SY = 96
SZ = 128
IF_DEV = 16
MAXSUB = 8
GROUPS = 4
NX = 64
NODES_DEV = 24576
IFACE = 512
LAM = 2048
N_DOM = 32


def draw_stiffness(key, part):
    base = jax.random.normal(jax.random.fold_in(key, 5), (GROUPS, 24, 24), jnp.float32) / math.sqrt(24.0)
    return jnp.einsum('gik,gjk->gij', base, base)


def pick_nodes(key, salt):
    keys = jax.random.split(jax.random.fold_in(key, salt), GROUPS * N_DOM)

    def single(one_key):
        return jax.random.permutation(one_key, NODES_DEV)[:IF_DEV]
    picks = jax.vmap(single)(keys)
    return picks.reshape(GROUPS, IFACE).astype(jnp.int32)


def draw_own_nodes(key, part):
    return pick_nodes(key, 11)


def draw_peer_nodes(key, part):
    return pick_nodes(key, 23)


def draw_schur_inverse(key, part):
    base = jax.random.normal(jax.random.fold_in(key, 1), (LAM, LAM), jnp.float32) * (0.5 / math.sqrt(LAM))
    sym = (base + base.T) * 0.5
    diag = jnp.exp(jax.random.uniform(jax.random.fold_in(key, 2), (LAM,), jnp.float32, math.log(0.5), math.log(2.0)))
    return sym + jnp.diag(diag)


def with_ends(entries, key, smallest, largest):
    place = [jax.random.randint(jax.random.fold_in(key, axis), (), 0, length) for axis, length in enumerate(entries.shape)]
    widest = entries.shape.index(max(entries.shape))
    neighbour = place[:widest] + [(place[widest] + 1) % entries.shape[widest]] + place[widest + 1:]
    return entries.at[tuple(place)].set(smallest).at[tuple(neighbour)].set(largest)


def steps_of(key, shape, cuts, low, high):
    level = 1.0
    for dim, shards_of in cuts:
        heights = jax.random.uniform(jax.random.fold_in(jax.random.fold_in(key, 6), dim), (shards_of,), jnp.float32, low / len(cuts), high / len(cuts))
        level = level * jnp.repeat(jnp.exp(heights), shape[dim] // shards_of).reshape((-1,) + (1,) * (len(shape) - 1 - dim))
    return level


def scatter_about(key, extent, scale, reach, cuts=(), kind=jnp.bfloat16):
    level = steps_of(key, extent, cuts, -0.22, 0.18) if cuts else 1.0
    entries = jax.random.normal(key, extent, jnp.float32) * scale * level
    return jnp.minimum(jnp.maximum(entries, -reach), reach).astype(kind)


def setup_inputs(seed: int = 0) -> dict:
    streams_of = jax.random.split(jax.random.key(seed), 12)
    displacement = scatter_about(streams_of[0], (GROUPS, 3, NX, SY, SZ), 0.5, 3.0, ((0, 4), (2, 32)), jnp.float32)
    velocity = scatter_about(streams_of[1], (GROUPS, 3, NX, SY, SZ), 1.0, 6.0, ((0, 4), (2, 32)), jnp.float32)
    external = scatter_about(streams_of[2], (GROUPS, 3, NX, SY, SZ), 1.0, 6.0, ((0, 4), (2, 32)), jnp.float32)
    mass = jnp.clip(jnp.exp(math.log(3.0) - 1.0986123 * jax.random.uniform(streams_of[3], (GROUPS, NX, SY, SZ), jnp.float32) ** steps_of(streams_of[3], (GROUPS, NX, SY, SZ), ((0, 4), (1, 32)), -0.2, 0.2)), 1.0, 3.0)
    elem_scale = jnp.clip(jnp.exp(math.log(0.5) - 2.3025851 * jax.random.uniform(streams_of[4], (GROUPS, NX, SY, SZ), jnp.float32) ** steps_of(streams_of[4], (GROUPS, NX, SY, SZ), ((0, 4), (1, 32)), -0.2, 0.2)), 0.05, 0.5)
    stiffness = draw_stiffness(jax.random.fold_in(streams_of[11], 71), 0)
    substeps = with_ends(jax.random.randint(streams_of[6], (GROUPS,), 1, MAXSUB + 1), jax.random.fold_in(streams_of[6], 1), 1, MAXSUB).astype(jnp.int32)
    own_nodes = draw_own_nodes(jax.random.fold_in(streams_of[11], 71), 0)
    peer_nodes = draw_peer_nodes(jax.random.fold_in(streams_of[11], 71), 0)
    normals = scatter_about(streams_of[9], (GROUPS, 3, IFACE), 1.0, 4.0, ((0, 4), (2, 32)), jnp.float32)
    schur_inverse = draw_schur_inverse(jax.random.fold_in(streams_of[11], 71), 0)
    return dict(displacement=displacement, velocity=velocity, external=external, mass=mass, elem_scale=elem_scale, stiffness=stiffness, substeps=substeps, own_nodes=own_nodes, peer_nodes=peer_nodes, normals=normals, schur_inverse=schur_inverse)


coarse_step = 0.4


def corner_stack(padded, planes):
    pieces = []
    for plane_off in (0, 1):
        for row_off in (0, 1):
            for col_off in (0, 1):
                block = padded[:, plane_off:plane_off + planes]
                block = jnp.roll(block, -row_off, axis=2)
                pieces.append(jnp.roll(block, -col_off, axis=3))
    return jnp.stack(pieces, 0).reshape(24, -1)


def element_forces(padded, scale, kmat):
    stacked = corner_stack(padded, scale.shape[0])
    forces = jnp.dot(kmat, stacked, precision=lax.Precision.HIGHEST, preferred_element_type=jnp.float32)
    forces = forces * scale.reshape(1, -1)
    return forces.reshape((8, 3) + scale.shape)


def assemble(forces):
    planes = forces.shape[2]
    total = jnp.zeros((3, planes + 1) + forces.shape[3:], jnp.float32)
    corner = 0
    for plane_off in (0, 1):
        for row_off in (0, 1):
            for col_off in (0, 1):
                part = jnp.roll(jnp.roll(forces[corner], row_off, axis=2), col_off, axis=3)
                total = total + jnp.pad(part, ((0, 0), (plane_off, 1 - plane_off), (0, 0), (0, 0)))
                corner = corner + 1
    return total


def group_internal(field, scale, kmat):
    padded = jnp.concatenate([field, jnp.zeros_like(field[:, :1])], 1)
    return assemble(element_forces(padded, scale, kmat))[:, :-1]


def reference(displacement, velocity, external, mass, elem_scale, stiffness, substeps, own_nodes, peer_nodes, normals, schur_inverse):
    fields = []
    speeds = []
    for group in range(GROUPS):
        delta = coarse_step / substeps[group].astype(jnp.float32)
        loads = external[group]
        weight = mass[group]
        scale = elem_scale[group]
        kmat = stiffness[group]

        def advance(step, state, loads=loads, weight=weight, scale=scale, kmat=kmat, delta=delta):
            field, speed = state
            accel = (loads - group_internal(field, scale, kmat)) / weight
            speed = speed + delta * accel
            field = field + delta * speed
            return field, speed

        field, speed = lax.fori_loop(0, substeps[group], advance, (displacement[group], velocity[group]))
        fields.append(field)
        speeds.append(speed.reshape(3, -1))
    offsets = (jnp.arange(N_DOM, dtype=jnp.int32) * NODES_DEV)[:, None]
    own_global = [(own_nodes[g].reshape(N_DOM, IF_DEV) + offsets).reshape(-1) for g in range(GROUPS)]
    peer_global = [(peer_nodes[g].reshape(N_DOM, IF_DEV) + offsets).reshape(-1) for g in range(GROUPS)]
    gaps = []
    for group in range(GROUPS):
        later = (group + 1) % GROUPS
        diff = speeds[group][:, own_global[group]] - speeds[later][:, peer_global[later]]
        gaps.append(jnp.sum(normals[group] * diff, axis=0))
    gap = jnp.concatenate(gaps, 0)
    multiplier = jnp.dot(schur_inverse, gap, precision=lax.Precision.HIGHEST, preferred_element_type=jnp.float32)
    multiplier = multiplier.reshape(GROUPS, IFACE)
    results = []
    for group in range(GROUPS):
        earlier = (group - 1) % GROUPS
        masses = mass[group].reshape(-1)
        correction = multiplier[group][None, :] * normals[group]
        incoming = multiplier[earlier][None, :] * normals[earlier]
        speed = speeds[group]
        speed = speed.at[:, own_global[group]].add(-correction / masses[own_global[group]][None, :])
        speed = speed.at[:, peer_global[group]].add(incoming / masses[peer_global[group]][None, :])
        results.append(speed.reshape(3, NX, SY, SZ))
    return jnp.stack(fields, 0), jnp.stack(results, 0)
```

```python
import jax
import jax.numpy as jnp
import numpy as np
from jax import lax
from jax.experimental import pallas as pl
from jax.experimental.pallas import tpu as pltpu
from jax.sharding import PartitionSpec as P

MAXSUB = 8
COARSE = 0.4
ROWS = 96
COLS = 128
SLOTS = 18
WROW = 4 * SLOTS
DUP = 56
F32 = jnp.float32
VM = pl.BlockSpec(memory_space=pltpu.VMEM)
SM = pl.BlockSpec(memory_space=pltpu.SMEM)


def selectors():
    pick_row = np.zeros((128, 24), np.float32)
    pick_col = np.zeros((2, 24, 256), np.float32)
    keep = np.zeros((2, 128, 256), np.float32)
    cols = []
    for part in range(4):
        b = part % 2
        width = WROW if part < 2 else DUP
        for k in range(width):
            kind, i = divmod(k, SLOTS)
            used = part < 2 or kind < 2
            cols.append((b, kind % 2, i // 3 - 2, i % 3) if used else None)
    for k, slot in enumerate(cols):
        if slot is None:
            continue
        b, e, plane, comp = slot
        for a in (0, 1):
            pick_col[a, (4 * a + 2 * b + e) * 3 + comp, k] = 1.0
    for tile in range(2):
        for g in range(8):
            for q in range(6):
                comp, x = divmod(q, 2)
                plane = x if tile == 0 else (-1 if x == 0 else 2)
                layer = plane - g // 4
                m = tile * 64 + g * 8 + q
                pick_row[m, g * 3 + comp] = 1.0
                for k, slot in enumerate(cols):
                    if slot is not None and slot[2] - layer in (0, 1):
                        keep[slot[2] - layer, m, k] = 1.0
    return pick_row, pick_col, keep


PICK_ROW, PICK_COL, KEEP = selectors()


def step_size(count_ref):
    count = jnp.full((8, COLS), count_ref[0], jnp.int32).astype(F32)
    return COARSE / count


def lane_up(x):
    return pltpu.roll(x, COLS - 1, 1)


def lane_down(x):
    return pltpu.roll(x, 1, 1)


def pack_body(parity_ref, u, v, ext, mass, scale, x_out, d_out):
    odd = parity_ref[0] == 1
    for q in range(6):
        x_out[q] = u[q]
        d_out[q] = u[q]
    for p in range(2):
        x_out[6 + p] = scale[p]
        d_out[6 + p] = scale[p]
    for c in range(3):
        for base, src in ((8, v), (11, ext)):
            lo, hi = src[2 * c], src[2 * c + 1]
            x_out[base + c] = jnp.where(odd, hi, lo)
            d_out[base + c] = jnp.where(odd, lo, hi)
    x_out[14] = jnp.where(odd, mass[1], mass[0])
    d_out[14] = jnp.where(odd, mass[0], mass[1])


def every(i, stride):
    return pl.ds(i, ROWS, stride=stride)


def prep_body(count_ref, v, ext, mass, kmat, pick_row, pick_col, keep, w_out, e_out, m_out, a_out):
    dt = step_size(count_ref)[0:1]
    for p in range(2):
        inv = (dt * dt) / mass[p]
        for c in range(3):
            q = 2 * c + p
            w_out[every(q, 8), :] = dt * v[q]
            e_out[every(q, 8), :] = inv * ext[q]
            m_out[every(q, 8), :] = inv
    zero = jnp.zeros((ROWS, COLS), F32)
    for q in (6, 7):
        w_out[every(q, 8), :] = zero
        e_out[every(q, 8), :] = zero
        m_out[every(q, 8), :] = zero
    high = lax.Precision.HIGHEST
    rows = jnp.dot(pick_row[...], kmat[...], precision=high, preferred_element_type=F32)
    full = keep[0] * jnp.dot(rows, pick_col[0], precision=high, preferred_element_type=F32)
    full = full + keep[1] * jnp.dot(rows, pick_col[1], precision=high, preferred_element_type=F32)
    big = full.astype(jnp.bfloat16).astype(F32)
    slot = lax.broadcasted_iota(jnp.int32, (128, 256), 1)
    a_out[...] = jnp.where(slot < 2 * WROW, big, full - big)


def build(wk, i, arr):
    lo = arr - arr.astype(jnp.bfloat16).astype(F32)
    for kind, val in enumerate((arr, lane_up(arr), lo, lane_up(lo))):
        wk[every(kind * SLOTS + i, WROW), :] = val


def one_step(wk, a_ref, tiles, s0, s1, act, e, m, w_in, u_in, w_out, u_out):
    nt = len(tiles)
    lhs = a_ref[0 : 64 * nt, :]
    wk[ROWS * WROW : (ROWS + 1) * WROW, :] = wk[0:WROW, :]

    def finish(t, r, force):
        at = slice(8 * r, 8 * r + 8)
        w = w_in[t][at, :] + act * (e[t][at, :] - m[t][at, :] * force)
        if w_out[t] is not None:
            w_out[t][at, :] = w
        u_out[t][at, :] = u_in[t][at, :] + act * w

    carry = {}
    first = {}
    for i in range(ROWS // 2):
        sides = []
        for r in (i, i + ROWS // 2):
            base = r * WROW
            sides.append(
                jnp.concatenate(
                    [
                        wk[base : base + 2 * WROW, :],
                        wk[base : base + DUP, :],
                        wk[base + WROW : base + WROW + DUP, :],
                    ],
                    0,
                )
            )
        out = jnp.dot(lhs, jnp.concatenate(sides, 1), preferred_element_type=F32)
        for h in range(2):
            r = i + h * (ROWS // 2)
            at = slice(8 * r, 8 * r + 8)
            for n, t in enumerate(tiles):
                lower, upper = s0[t][at, :], s1[t][at, :]

                def block(g):
                    j = 64 * n + 8 * g
                    return out[j : j + 8, h * COLS : (h + 1) * COLS]

                part = []
                for b in range(2):
                    g0 = lower * block(2 * b) + upper * block(4 + 2 * b)
                    g1 = lower * block(2 * b + 1) + upper * block(5 + 2 * b)
                    part.append(g0 + lane_down(g1))
                if i == 0:
                    first[h, t] = part[0]
                else:
                    finish(t, r, part[0] + carry[h, t])
                carry[h, t] = part[1]
    for t in tiles:
        finish(t, 0, first[0, t] + carry[1, t])
        finish(t, ROWS // 2, first[1, t] + carry[0, t])


def two_steps(rnd, count_ref, u_nat, lower, upper, refs):
    wk, a_ref, s0, s1, e, m, w_in, w_tmp, u_cur, w_halo, u_mid, w_out, u_new, u_out, u_prev = refs
    act = [jnp.where(count_ref[0] > 2 * rnd + k, 1.0, 0.0).astype(F32) for k in range(2)]
    for c in range(3):
        for p in range(2):
            own = u_nat[2 * c + p]
            build(wk, (p + 2) * 3 + c, own)
            u_cur[0][every(2 * c + p, 8), :] = own
            low = lower(2 * c + p)
            build(wk, p * 3 + c, low)
            top = upper(2 * c + p)
            build(wk, (p + 4) * 3 + c, top)
            if p == 1:
                u_cur[1][every(2 * c, 8), :] = low
            else:
                u_cur[1][every(2 * c + 1, 8), :] = top
    if rnd > 0:
        for r in range(ROWS):
            at = slice(8 * r, 8 * r + 8)
            w_halo[at, :] = u_cur[1][at, :] - u_prev[at, :]
    one_step(wk, a_ref, (0, 1), s0, s1, act[0], e, m, (w_in, w_halo), u_cur, (w_tmp, None), u_mid)
    for c in range(3):
        for p in range(2):
            build(wk, (p + 2) * 3 + c, u_mid[0][every(2 * c + p, 8), :])
            build(wk, (1 if p == 0 else 4) * 3 + c, u_mid[1][every(2 * c + p, 8), :])
    one_step(wk, a_ref, (0,), s0, s1, act[1], e, m, (w_tmp,), (u_mid[0],), (w_out,), (u_new,))
    for q in range(6):
        u_out[q] = u_new[every(q, 8), :]


def first_body(
    count_ref, parity_ref, u_nat, scale, x_in, d_in, w_in, e_own, m_own, a_ref,
    u_out, w_out, u_keep, s_out, eh_out, mh_out,
    wk, w_tmp, u_cur, w_halo, u_mid, u_new,
):
    odd = parity_ref[0] == 1
    dt = step_size(count_ref)[0:1]

    def lower(k):
        return jnp.where(odd, d_in[k], x_in[k])

    def upper(k):
        return jnp.where(odd, x_in[k], d_in[k])

    layers = {-2: lower(6), -1: lower(7), 0: scale[0], 1: scale[1], 2: upper(6)}
    zero = jnp.zeros((ROWS, COLS), F32)
    for q in (6, 7):
        for ref in (s_out.at[0], s_out.at[1], s_out.at[2], s_out.at[3], eh_out, mh_out, w_halo, u_cur.at[0], u_cur.at[1]):
            ref[every(q, 8), :] = zero
    for c in range(3):
        for x in range(2):
            q = 2 * c + x
            outer = -1 if x == 0 else 2
            s_out.at[0][every(q, 8), :] = layers[x]
            s_out.at[1][every(q, 8), :] = layers[x - 1]
            s_out.at[2][every(q, 8), :] = layers[outer]
            s_out.at[3][every(q, 8), :] = layers[outer - 1]
            get = lower if x == 0 else upper
            weight = get(14)
            inv = jnp.where(weight > 0.0, (dt * dt) / jnp.where(weight > 0.0, weight, 1.0), 0.0)
            mh_out[every(q, 8), :] = inv
            eh_out[every(q, 8), :] = inv * get(11 + c)
            w_halo[every(q, 8), :] = dt * get(8 + c)
    s0 = (s_out.at[0], s_out.at[2])
    s1 = (s_out.at[1], s_out.at[3])
    refs = (
        wk, a_ref, s0, s1, (e_own, eh_out), (m_own, mh_out), w_in, w_tmp,
        (u_cur.at[0], u_cur.at[1]), w_halo, (u_mid, u_keep), w_out, u_new, u_out, None,
    )
    two_steps(0, count_ref, u_nat, lower, upper, refs)


def next_body(
    rnd,
    count_ref, parity_ref, u_nat, x_in, d_in, w_in, u_prev, s_in, e_own, eh, m_own, mh, a_ref,
    u_out, w_out, u_keep,
    wk, w_tmp, u_cur, w_halo, u_mid, u_new,
):
    odd = parity_ref[0] == 1

    def lower(k):
        return jnp.where(odd, d_in[k], x_in[k])

    def upper(k):
        return jnp.where(odd, x_in[k], d_in[k])

    zero = jnp.zeros((ROWS, COLS), F32)
    for q in (6, 7):
        for ref in (u_cur.at[0], u_cur.at[1]):
            ref[every(q, 8), :] = zero
    s0 = (s_in.at[0], s_in.at[2])
    s1 = (s_in.at[1], s_in.at[3])
    refs = (
        wk, a_ref, s0, s1, (e_own, eh), (m_own, mh), w_in, w_tmp,
        (u_cur.at[0], u_cur.at[1]), w_halo, (u_mid, u_keep), w_out, u_new, u_out, u_prev,
    )
    two_steps(rnd, count_ref, u_nat, lower, upper, refs)


def node_of(index):
    plane = index // (ROWS * COLS)
    row = (index // COLS) % ROWS
    return plane, row, index % COLS


def node_weights(plane, col, normal, j):
    sub = lax.broadcasted_iota(jnp.int32, (8, COLS), 0)
    lane = lax.broadcasted_iota(jnp.int32, (8, COLS), 1)
    weight = jnp.zeros((8, COLS), F32)
    for c in range(3):
        hit = (sub == 2 * c + plane) & (lane == col)
        weight = jnp.where(hit, normal[c, j], weight)
    return weight


def gap_body(count_ref, slice_ref, own, peer, normal, before, w_in, g_out, hits):
    dt = step_size(count_ref)
    eighth = slice_ref[0] % 8
    for side, nodes, vec, sign in ((0, own, normal, 1.0), (1, peer, before, -1.0)):
        for j in range(16):
            plane, row, col = node_of(nodes[j])
            tile = w_in[pl.ds(pl.multiple_of(row * 8, 8), 8), :]
            hits[side * 16 + j] = tile * node_weights(plane, col, vec, j)
        total = jnp.sum(hits[side * 16 : side * 16 + 16], axis=1)
        total = jnp.sum(total, axis=1, keepdims=True) * (sign / dt[0:1, 0:1])
        lane = lax.broadcasted_iota(jnp.int32, (16, COLS), 1)
        sub = lax.broadcasted_iota(jnp.int32, (16, COLS), 0)
        line = jnp.where(lane == sub + 16 * eighth, jnp.broadcast_to(total, (16, COLS)), 0.0)
        line = jnp.sum(line, axis=0, keepdims=True)
        g_out[:, side * COLS : (side + 1) * COLS] = jnp.broadcast_to(line, (128, COLS))


def final_body(
    count_ref, own, peer, normal, before, gathered, inv_own, inv_before, w_in, m_own, u_dummy,
    v_out, work, mult,
):
    dt = step_size(count_ref)
    mine = jnp.sum(gathered[:, 0:COLS].reshape(16, 8, COLS), axis=1)
    other = jnp.sum(gathered[:, COLS : 2 * COLS].reshape(16, 8, COLS), axis=1)
    gap = mine + jnp.concatenate([other[4:16], other[0:4]], 0)
    for side, rows in ((0, inv_own), (1, inv_before)):
        acc = jnp.zeros((16, COLS), F32)
        for k in range(16):
            acc = acc + rows[:, k * COLS : (k + 1) * COLS] * gap[k : k + 1, :]
        lam = jnp.sum(acc, axis=1, keepdims=True)
        mult[side * 16 : side * 16 + 16, :] = jnp.broadcast_to(lam, (16, COLS))
    work[...] = w_in[...]
    for side, nodes, vec, sign in ((0, own, normal, -1.0), (1, peer, before, 1.0)):
        for j in range(16):
            plane, row, col = node_of(nodes[j])
            at = pl.ds(pl.multiple_of(row * 8, 8), 8)
            k = side * 16 + j
            scaled = mult[k : k + 1, :] * (sign / dt[0:1])
            work[at, :] = work[at, :] + node_weights(plane, col, vec, j) * m_own[at, :] * scaled
    back = 1.0 / dt[0:1]
    for q in range(6):
        v_out[q] = work[every(q, 8), :] * back


def call(body, outs, scratch, ins, limit=24 * 1024 * 1024):
    return pl.pallas_call(
        body,
        out_shape=[jax.ShapeDtypeStruct(s, F32) for s in outs],
        in_specs=ins,
        out_specs=[VM] * len(outs),
        scratch_shapes=[pltpu.VMEM(s, F32) for s in scratch],
        compiler_params=pltpu.CompilerParams(vmem_limit_bytes=limit),
    )


TILE = (ROWS * 8, COLS)
PLANES = (6, ROWS, COLS)
WORK = [((ROWS + 1) * WROW, COLS), TILE, (2,) + TILE, TILE, TILE, TILE]
ACROSS = [(i, i + 1) for i in range(1, 31, 2)] + [(i + 1, i) for i in range(1, 31, 2)]
WITHIN = [(i, i ^ 1) for i in range(32)]
FROM_BEFORE = [(i, (i + 1) % 4) for i in range(4)]


def on_device(
    displacement, velocity, external, mass, elem_scale, stiffness, substeps,
    own_nodes, peer_nodes, normals, schur_inverse,
):
    field = displacement[0].reshape(PLANES)
    speed = velocity[0].reshape(PLANES)
    loads = external[0].reshape(PLANES)
    weight = mass[0]
    scale = elem_scale[0]
    place = lax.axis_index("dom").reshape(1)
    parity = place % 2
    own = own_nodes[0]
    peer = peer_nodes[0]
    normal = normals[0]

    def exchange(x, d):
        return lax.ppermute(x, "dom", ACROSS), lax.ppermute(d, "dom", WITHIN)

    msg = (15, ROWS, COLS)
    x, d = call(pack_body, [msg, msg], [], [SM] + [VM] * 5)(parity, field, speed, loads, weight, scale)
    x, d = exchange(x, d)
    inv_before = lax.ppermute(schur_inverse, "grp", FROM_BEFORE)
    before = lax.ppermute(normal, "grp", FROM_BEFORE)
    w, e_own, m_own, a = call(
        prep_body, [TILE, TILE, TILE, (128, 256)], [], [SM] + [VM] * 7
    )(substeps, speed, loads, weight, stiffness[0], PICK_ROW, PICK_COL, KEEP)
    u, w, kept, s, eh, mh = call(
        first_body, [PLANES, TILE, TILE, (4,) + TILE, TILE, TILE], WORK, [SM] * 2 + [VM] * 8
    )(substeps, parity, field, scale, x, d, w, e_own, m_own, a)
    for rnd in range(1, MAXSUB // 2):
        x, d = exchange(u, u)

        def body(*refs, rnd=rnd):
            return next_body(rnd, *refs)

        u, w, kept = call(body, [PLANES, TILE, TILE], WORK, [SM] * 2 + [VM] * 11)(
            substeps, parity, u, x, d, w, kept, s, e_own, eh, m_own, mh, a
        )
    (gap,) = call(gap_body, [(128, 2 * COLS)], [(32, 8, COLS)], [SM] * 6 + [VM])(
        substeps, place, own, peer, normal, before, w
    )
    gathered = lax.all_to_all(gap, ("grp", "dom"), 0, 0, tiled=True)
    (v,) = call(
        final_body, [PLANES], [TILE, (32, COLS)], [SM] * 5 + [VM] * 6
    )(substeps, own, peer, normal, before, gathered, schur_inverse, inv_before, w, m_own, m_own)
    shape = displacement.shape
    return u.reshape(shape), v.reshape(shape)


def solution(mesh):
    return jax.shard_map(
        on_device,
        mesh=mesh,
        in_specs=(
            P("grp", None, "dom", None, None),
            P("grp", None, "dom", None, None),
            P("grp", None, "dom", None, None),
            P("grp", "dom", None, None),
            P("grp", "dom", None, None),
            P("grp", None, None),
            P("grp"),
            P("grp", "dom"),
            P("grp", "dom"),
            P("grp", None, "dom"),
            P(("grp", "dom"), None),
        ),
        out_specs=(P("grp", None, "dom", None, None), P("grp", None, "dom", None, None)),
        check_vma=False,
    )
```

```python
import jax
import jax.numpy as jnp
import numpy as np
from jax import lax
from jax.experimental import pallas as pl
from jax.experimental.pallas import tpu as pltpu
from jax.sharding import PartitionSpec as P

MAXSUB = 8
ROUNDS = MAXSUB // 2
COARSE = 0.4
ROWS = 96
HALF = ROWS // 2
COLS = 128
WROW = 56
STEP_PARTS = [(0, 48), (WROW, 48), (0, 16), (24, 16), (WROW, 16), (WROW + 24, 16)]
INNER_PARTS = [(0, 24), (WROW, 24), (0, 16), (WROW, 16)]
STEP_K, INNER_K = 256, 128
F32 = jnp.float32
VM = pl.BlockSpec(memory_space=pltpu.VMEM)
SM = pl.BlockSpec(memory_space=pltpu.SMEM)
HBM = pl.BlockSpec(memory_space=pl.ANY)


def describe(parts, width):
    cols = []
    for n, (start, size) in enumerate(parts):
        for at in range(start, start + size):
            b, at = divmod(at, WROW)
            outer, at = divmod(at, 24)
            kind, at = divmod(at, 6)
            x, comp = divmod(at, 3)
            plane = (-1 if x == 0 else 2) if outer else x
            cols.append((b, kind % 2, plane, comp) if n < 2 or kind < 2 else None)
    return cols + [None] * (width - len(cols))


def selectors():
    cols = describe(STEP_PARTS, STEP_K) + describe(INNER_PARTS, INNER_K)
    pick_row = np.zeros((96, 24), np.float32)
    pick_col = np.zeros((2, 24, len(cols)), np.float32)
    keep = np.zeros((2, 96, len(cols)), np.float32)
    for k, slot in enumerate(cols):
        if slot is not None:
            b, e, plane, comp = slot
            for a in (0, 1):
                pick_col[a, (4 * a + 2 * b + e) * 3 + comp, k] = 1.0
    for block in range(3):
        for be in range(4):
            for q in range(6):
                comp, x = divmod(q, 2)
                layer = 0 if block == 0 else (-1 if x == 0 else 1)
                a = 1 - x if block == 1 else x
                m = block * 32 + be * 8 + q
                pick_row[m, (4 * a + be) * 3 + comp] = 1.0
                for k, slot in enumerate(cols):
                    if slot is not None and slot[2] - layer in (0, 1):
                        keep[slot[2] - layer, m, k] = 1.0
    return pick_row, pick_col, keep


PICK_ROW, PICK_COL, KEEP = selectors()


def step_size(count_ref):
    count = jnp.full((8, COLS), count_ref[0], jnp.int32).astype(F32)
    return COARSE / count


def lane_up(x):
    return pltpu.roll(x, COLS - 1, 1)


def lane_down(x):
    return pltpu.roll(x, 1, 1)


def every(i, stride=8):
    return pl.ds(i, ROWS, stride=stride)


def tile(r):
    return slice(8 * r, 8 * r + 8)


def build(wk, outer, i, arr):
    lo = arr - arr.astype(jnp.bfloat16).astype(F32)
    for kind, val in enumerate((arr, lane_up(arr), lo, lane_up(lo))):
        wk[every(outer * 24 + kind * 6 + i, WROW), :] = val


def sweep(wk, lhs, parts, width, blocks, finish):
    wk[ROWS * WROW : (ROWS + 1) * WROW, :] = wk[0:WROW, :]
    pad = jnp.zeros((width - sum(n for _, n in parts), COLS), F32)
    carry = {}
    first = {}
    for i in range(HALF):
        sides = []
        for r in (i, i + HALF):
            base = r * WROW
            pieces = [wk[base + at : base + at + n, :] for at, n in parts]
            sides.append(jnp.concatenate(pieces + [pad], 0))
        out = jnp.dot(lhs, jnp.concatenate(sides, 1), preferred_element_type=F32)
        for h in range(2):
            r = i + h * HALF
            for n, terms in enumerate(blocks):
                part = []
                for b in range(2):
                    g = []
                    for e in range(2):
                        total = None
                        for offset, scale in terms:
                            j = offset + 16 * b + 8 * e
                            term = scale[tile(r), :] * out[j : j + 8, h * COLS : (h + 1) * COLS]
                            total = term if total is None else total + term
                        g.append(total)
                    part.append(g[0] + lane_down(g[1]))
                if i == 0:
                    first[h, n] = part[0]
                else:
                    finish(n, r, part[0] + carry[h, n])
                carry[h, n] = part[1]
    for n in range(len(blocks)):
        finish(n, 0, first[0, n] + carry[1, n])
        finish(n, HALF, first[1, n] + carry[0, n])


def inner_pass(wk, a_ref, si, e, m, u, w, ei_out, h_out):
    def finish(n, r, force):
        at = tile(r)
        rest = e[at, :] - m[at, :] * force
        ei_out[at, :] = rest
        h_out[at, :] = u[at, :] + (w[at, :] + rest)

    sweep(wk, a_ref[0:32, STEP_K:], INNER_PARTS, INNER_K, [[(0, si)]], finish)


def send_edges(odd, u, h, x_msg, d_msg):
    for base, src in ((0, u), (3, h)):
        for c in range(3):
            low, top = src[every(2 * c), :], src[every(2 * c + 1), :]
            x_msg[base + c] = jnp.where(odd, top, low)
            d_msg[base + c] = jnp.where(odd, low, top)


def prep_body(
    count_ref, parity_ref, kmat_h, row_h, col_h, keep_h, u_h, scale_h, v_h, mass_h, ext_h,
    x_msg, d_msg, u_t, w_t, e_t, m_t, ei_t, si_t, a_out,
    kmat, row, col, keep, u_n, scale, v_n, mass, ext_n, wk, h_t, sems,
):
    pairs = [
        (kmat_h, kmat), (row_h, row), (col_h, col), (keep_h, keep), (u_h, u_n),
        (scale_h, scale), (v_h, v_n), (mass_h, mass), (ext_h, ext_n),
    ]
    copies = [pltpu.make_async_copy(a, b, sems.at[n]) for n, (a, b) in enumerate(pairs)]
    for copy in copies:
        copy.start()
    for copy in copies:
        copy.wait()
    odd = parity_ref[0] == 1
    dt = step_size(count_ref)[0:1]
    high = lax.Precision.HIGHEST
    rows = jnp.dot(row[...], kmat[...], precision=high, preferred_element_type=F32)
    full = keep[0] * jnp.dot(rows, col[0], precision=high, preferred_element_type=F32)
    full = full + keep[1] * jnp.dot(rows, col[1], precision=high, preferred_element_type=F32)
    big = full.astype(jnp.bfloat16).astype(F32)
    slot = lax.broadcasted_iota(jnp.int32, full.shape, 1)
    main = (slot < 96) | ((slot >= STEP_K) & (slot < STEP_K + 48))
    a_out[...] = jnp.where(main, big, full - big)
    inv = [(dt * dt) / mass[p] for p in range(2)]
    for c in range(3):
        for p in range(2):
            q = 2 * c + p
            build(wk, 0, 3 * p + c, u_n[q])
            u_t[every(q), :] = u_n[q]
            w_t[every(q), :] = dt * v_n[q]
            e_t[every(q), :] = inv[p] * ext_n[q]
            m_t[every(q), :] = inv[p]
            si_t[every(q), :] = scale[0]
    inner_pass(wk, a_out, si_t, e_t, m_t, u_t, w_t, ei_t, h_t)
    send_edges(odd, u_t, h_t, x_msg, d_msg)
    x_msg[6] = jnp.where(odd, inv[1], inv[0])
    d_msg[6] = jnp.where(odd, inv[0], inv[1])
    x_msg[7] = scale[1]
    d_msg[7] = scale[1]


def round_body(rnd, *refs):
    refs = list(refs)
    take = lambda n: [refs.pop(0) for _ in range(n)]
    count_ref, parity_ref = take(2)
    last = rnd == ROUNDS - 1
    if last:
        place_ref, own, peer, normal, before = take(5)
    x_in, d_in, u_t, w_t, e_t, m_t, ei_t, si_t, a_ref = take(9)
    if rnd == 0:
        (scale,) = take(1)
    else:
        sx_t, mh_t = take(2)
    if last:
        u_out, w2, g_out = take(3)
    else:
        x_msg, d_msg, u2, w2, ei_out = take(5)
    if rnd == 0:
        sx_t, mh_t = take(2)
    wk, uh, hh, u1, u1h, w1, h_t = take(7)
    if last:
        u2, hits = take(2)
    odd = parity_ref[0] == 1

    def lower(k):
        return jnp.where(odd, d_in[k], x_in[k])

    def upper(k):
        return jnp.where(odd, x_in[k], d_in[k])

    act = [jnp.where(count_ref[0] > 2 * rnd + k, 1.0, 0.0).astype(F32) for k in range(2)]
    for c in range(3):
        for p, get in ((0, lower), (1, upper)):
            q = 2 * c + p
            build(wk, 0, 3 * p + c, u_t[every(q), :])
            outer = get(c)
            build(wk, 1, 3 * p + c, outer)
            uh[every(q), :] = outer
            hh[every(q), :] = get(3 + c)
            if rnd == 0:
                mh_t[every(q), :] = get(6)
                sx_t[every(q), :] = scale[1] if p else lower(7)

    def finish_first(n, r, force):
        at = tile(r)
        if n == 0:
            w = w_t[at, :] + act[0] * (ei_t[at, :] - m_t[at, :] * force)
            w1[at, :] = w
            u1[at, :] = u_t[at, :] + act[0] * w
        else:
            before = uh[at, :]
            u1h[at, :] = before + act[0] * ((hh[at, :] - mh_t[at, :] * force) - before)

    sweep(wk, a_ref[32:96, 0:STEP_K], STEP_PARTS, STEP_K, [[(0, sx_t)], [(32, sx_t)]], finish_first)
    for c in range(3):
        for p in range(2):
            build(wk, 0, 3 * p + c, u1[every(2 * c + p), :])
            build(wk, 1, 3 * p + c, u1h[every(2 * c + p), :])

    def finish_second(n, r, force):
        at = tile(r)
        w = w1[at, :] + act[1] * (e_t[at, :] - m_t[at, :] * force)
        w2[at, :] = w
        u2[at, :] = u1[at, :] + act[1] * w

    sweep(wk, a_ref[0:64, 0:STEP_K], STEP_PARTS, STEP_K, [[(0, si_t), (32, sx_t)]], finish_second)
    if last:
        for q in range(6):
            u_out[q] = u2[every(q), :]
        partial_gaps(count_ref, place_ref, own, peer, normal, before, w2, g_out, hits)
        return
    for c in range(3):
        for p in range(2):
            build(wk, 0, 3 * p + c, u2[every(2 * c + p), :])
    inner_pass(wk, a_ref, si_t, e_t, m_t, u2, w2, ei_out, h_t)
    send_edges(odd, u2, h_t, x_msg, d_msg)


def node_of(index):
    plane = index // (ROWS * COLS)
    row = (index // COLS) % ROWS
    return plane, pl.ds(pl.multiple_of(row * 8, 8), 8), index % COLS


def node_hits(plane, col):
    sub = lax.broadcasted_iota(jnp.int32, (8, COLS), 0)
    lane = lax.broadcasted_iota(jnp.int32, (8, COLS), 1)
    return [(sub == 2 * c + plane) & (lane == col) for c in range(3)]


def partial_gaps(count_ref, place_ref, own, peer, normal, before, w_in, g_out, hits):
    dt = step_size(count_ref)
    eighth = place_ref[0] % 8
    for side, nodes, vec, sign in ((0, own, normal, 1.0), (1, peer, before, -1.0)):
        for j in range(16):
            plane, at, col = node_of(nodes[j])
            value = w_in[at, :]
            total = jnp.zeros((8, COLS), F32)
            for c, hit in enumerate(node_hits(plane, col)):
                total = jnp.where(hit, value * vec[c, j], total)
            hits[side * 16 + j] = total
        total = jnp.sum(hits[side * 16 : side * 16 + 16], axis=1)
        total = jnp.sum(total, axis=1, keepdims=True) * (sign / dt[0:1, 0:1])
        lane = lax.broadcasted_iota(jnp.int32, (16, COLS), 1)
        sub = lax.broadcasted_iota(jnp.int32, (16, COLS), 0)
        line = jnp.where(lane == sub + 16 * eighth, jnp.broadcast_to(total, (16, COLS)), 0.0)
        line = jnp.sum(line, axis=0, keepdims=True)
        g_out[:, side * COLS : (side + 1) * COLS] = jnp.broadcast_to(line, (128, COLS))


def final_body(
    count_ref, own, peer, normal, before, gathered, inv_own, inv_before, w_in, m_own,
    v_out, work, mult,
):
    dt = step_size(count_ref)
    mine = jnp.sum(gathered[:, 0:COLS].reshape(16, 8, COLS), axis=1)
    other = jnp.sum(gathered[:, COLS : 2 * COLS].reshape(16, 8, COLS), axis=1)
    gap = mine + jnp.concatenate([other[4:16], other[0:4]], 0)
    for side, rows in ((0, inv_own), (1, inv_before)):
        acc = jnp.zeros((16, COLS), F32)
        for k in range(16):
            acc = acc + rows[:, k * COLS : (k + 1) * COLS] * gap[k : k + 1, :]
        lam = jnp.sum(acc, axis=1, keepdims=True)
        mult[side * 16 : side * 16 + 16, :] = jnp.broadcast_to(lam, (16, COLS))
    work[...] = w_in[...]
    for side, nodes, vec, sign in ((0, own, normal, -1.0), (1, peer, before, 1.0)):
        for j in range(16):
            plane, at, col = node_of(nodes[j])
            k = side * 16 + j
            value = work[at, :]
            change = m_own[at, :] * (mult[k : k + 1, :] * (sign / dt[0:1]))
            for c, hit in enumerate(node_hits(plane, col)):
                value = jnp.where(hit, value + change * vec[c, j], value)
            work[at, :] = value
    back = 1.0 / dt[0:1]
    for q in range(6):
        v_out[q] = work[every(q), :] * back


def call(body, outs, scratch, ins, limit=24 * 1024 * 1024):
    return pl.pallas_call(
        body,
        out_shape=[jax.ShapeDtypeStruct(s, F32) for s in outs],
        in_specs=ins,
        out_specs=[VM] * len(outs),
        scratch_shapes=[pltpu.VMEM(s, F32) if isinstance(s, tuple) else s for s in scratch],
        compiler_params=pltpu.CompilerParams(vmem_limit_bytes=limit),
    )


TILE = (ROWS * 8, COLS)
PLANES = (6, ROWS, COLS)
WORK = ((ROWS + 1) * WROW, COLS)
WIDTH = STEP_K + INNER_K
ACROSS = [(i, i + 1) for i in range(1, 31, 2)] + [(i + 1, i) for i in range(1, 31, 2)]
WITHIN = [(i, i ^ 1) for i in range(32)]
FROM_BEFORE = [(i, (i + 1) % 4) for i in range(4)]


def on_device(
    displacement, velocity, external, mass, elem_scale, stiffness, substeps,
    own_nodes, peer_nodes, normals, schur_inverse,
):
    field = displacement[0].reshape(PLANES)
    speed = velocity[0].reshape(PLANES)
    loads = external[0].reshape(PLANES)
    weight = mass[0]
    scale = elem_scale[0]
    place = lax.axis_index("dom").reshape(1)
    parity = place % 2
    own = own_nodes[0]
    peer = peer_nodes[0]
    normal = normals[0]

    first = (8, ROWS, COLS)
    pair = (2, ROWS, COLS)
    x, d, u, w, e, m, ei, si, a = call(
        prep_body,
        [first, first, TILE, TILE, TILE, TILE, TILE, TILE, (96, WIDTH)],
        [
            (24, 24), (96, 24), (2, 24, WIDTH), (2, 96, WIDTH), PLANES, pair, PLANES, pair, PLANES,
            WORK, TILE, pltpu.SemaphoreType.DMA((9,)),
        ],
        [SM] * 2 + [HBM] * 9,
    )(substeps, parity, stiffness[0], PICK_ROW, PICK_COL, KEEP, field, scale, speed, weight, loads)
    inv_before = before = None
    for rnd in range(ROUNDS):
        x = lax.ppermute(x, "dom", ACROSS)
        d = lax.ppermute(d, "dom", WITHIN)
        if rnd == 0:
            inv_before = lax.ppermute(schur_inverse, "grp", FROM_BEFORE)
            before = lax.ppermute(normal, "grp", FROM_BEFORE)
        last = rnd == ROUNDS - 1
        args = [substeps, parity]
        if last:
            args += [place, own, peer, normal, before]
        scalars = len(args)
        args += [x, d, u, w, e, m, ei, si, a]
        args += [scale] if rnd == 0 else [sx, mh]
        outs = [PLANES, TILE, (128, 2 * COLS)] if last else [PLANES, PLANES, TILE, TILE, TILE]
        outs += [TILE, TILE] if rnd == 0 else []
        scratch = [WORK] + [TILE] * 6 + ([TILE, (32, 8, COLS)] if last else [])

        def body(*refs, rnd=rnd):
            return round_body(rnd, *refs)

        got = call(body, outs, scratch, [SM] * scalars + [VM] * (len(args) - scalars))(*args)
        if last:
            u, w, gap = got
        else:
            x, d, u, w, ei = got[:5]
        if rnd == 0:
            sx, mh = got[5:]
    gathered = lax.all_to_all(gap, ("grp", "dom"), 0, 0, tiled=True)
    (v,) = call(final_body, [PLANES], [TILE, (32, COLS)], [SM] * 5 + [VM] * 5)(
        substeps, own, peer, normal, before, gathered, schur_inverse, inv_before, w, m
    )
    shape = displacement.shape
    return u.reshape(shape), v.reshape(shape)


def solution(mesh):
    return jax.shard_map(
        on_device,
        mesh=mesh,
        in_specs=(
            P("grp", None, "dom", None, None),
            P("grp", None, "dom", None, None),
            P("grp", None, "dom", None, None),
            P("grp", "dom", None, None),
            P("grp", "dom", None, None),
            P("grp", None, None),
            P("grp"),
            P("grp", "dom"),
            P("grp", "dom"),
            P("grp", None, "dom"),
            P(("grp", "dom"), None),
        ),
        out_specs=(P("grp", None, "dom", None, None), P("grp", None, "dom", None, None)),
        check_vma=False,
    )
```

```python
import jax
import jax.numpy as jnp
import numpy as np
from jax import lax
from jax.experimental import pallas as pl
from jax.experimental.pallas import tpu as pltpu
from jax.sharding import PartitionSpec as P

MAXSUB = 8
ROUNDS = MAXSUB // 2
COARSE = 0.4
ROWS = 96
HALF = ROWS // 2
COLS = 128
STEP_K, INNER_K = 256, 128
F32 = jnp.float32
VM = pl.BlockSpec(memory_space=pltpu.VMEM)
SM = pl.BlockSpec(memory_space=pltpu.SMEM)
HBM = pl.BlockSpec(memory_space=pltpu.HBM)


def describe():
    cols = []
    for b, kinds in ((0, 4), (1, 4), (0, 2), (1, 2)):
        for kind in range(kinds):
            for q in range(16):
                x, comp = q % 2, (q % 8) // 2
                plane = x if q < 8 else (-1 if x == 0 else 2)
                cols.append((b, kind % 2, plane, comp) if q % 8 < 6 else None)
    cols += [None] * (STEP_K - len(cols))
    for kind in range(6):
        for q in range(16):
            cols.append((q // 8, kind % 2, q % 2, (q % 8) // 2) if q % 8 < 6 else None)
    return cols + [None] * (STEP_K + INNER_K - len(cols))


def selectors():
    cols = describe()
    pick_row = np.zeros((96, 24), np.float32)
    pick_col = np.zeros((2, 24, len(cols)), np.float32)
    keep = np.zeros((2, 96, len(cols)), np.float32)
    for k, slot in enumerate(cols):
        if slot is not None:
            b, e, plane, comp = slot
            for a in (0, 1):
                pick_col[a, (4 * a + 2 * b + e) * 3 + comp, k] = 1.0
    for block in range(3):
        for be in range(4):
            for q in range(6):
                comp, x = divmod(q, 2)
                layer = 0 if block == 0 else (-1 if x == 0 else 1)
                a = 1 - x if block == 1 else x
                m = block * 32 + be * 8 + q
                pick_row[m, (4 * a + be) * 3 + comp] = 1.0
                for k, slot in enumerate(cols):
                    if slot is not None and slot[2] - layer in (0, 1):
                        keep[slot[2] - layer, m, k] = 1.0
    return pick_row, pick_col, keep


PICK_ROW, PICK_COL, KEEP = selectors()


def step_size(count_ref):
    count = jnp.full((8, COLS), count_ref[0], jnp.int32).astype(F32)
    return COARSE / count


def lane_up(x):
    return pltpu.roll(x, COLS - 1, 1)


def lane_down(x):
    return pltpu.roll(x, 1, 1)


def every(i, stride=8):
    return pl.ds(i, ROWS, stride=stride)


def tile(r):
    return slice(8 * r, 8 * r + 8)


def split(u):
    hi = u.astype(jnp.bfloat16)
    lo = (u - hi.astype(F32)).astype(jnp.bfloat16)
    return [hi, lane_up(hi), lo, lane_up(lo)]


def step_rows(own, outer):
    done = {}

    def one(r):
        r %= ROWS
        if r not in done:
            done[r] = split(jnp.concatenate([own[tile(r), :], outer[tile(r), :]], 0))
        return done[r]

    def rows(r):
        here, there = one(r), one(r + 1)
        pad = jnp.zeros((64, COLS), jnp.bfloat16)
        return jnp.concatenate(here + there + here[:2] + there[:2] + [pad], 0)

    return rows


def inner_rows(own):
    def rows(r):
        parts = split(jnp.concatenate([own[tile(r), :], own[tile((r + 1) % ROWS), :]], 0))
        pad = jnp.zeros((32, COLS), jnp.bfloat16)
        return jnp.concatenate(parts + parts[:2] + [pad], 0)

    return rows


def sweep(rows, lhs, blocks, finish):
    carry = {}
    first = {}
    for i in range(HALF):
        rhs = jnp.concatenate([rows(i), rows(i + HALF)], 1)
        out = jnp.dot(lhs, rhs, preferred_element_type=F32)
        for h in range(2):
            r = i + h * HALF
            for n, terms in enumerate(blocks):
                part = []
                for b in range(2):
                    g = []
                    for e in range(2):
                        total = None
                        for offset, scale in terms:
                            j = offset + 16 * b + 8 * e
                            term = scale[tile(r), :] * out[j : j + 8, h * COLS : (h + 1) * COLS]
                            total = term if total is None else total + term
                        g.append(total)
                    part.append(g[0] + lane_down(g[1]))
                if i == 0:
                    first[h, n] = part[0]
                else:
                    finish(n, r, part[0] + carry[h, n])
                carry[h, n] = part[1]
    for n in range(len(blocks)):
        finish(n, 0, first[0, n] + carry[1, n])
        finish(n, HALF, first[1, n] + carry[0, n])


def inner_pass(a_ref, si, e, m, u, w, ei_out, h_out):
    def finish(n, r, force):
        at = tile(r)
        rest = e[at, :] - m[at, :] * force
        ei_out[at, :] = rest
        h_out[at, :] = u[at, :] + (w[at, :] + rest)

    sweep(inner_rows(u), a_ref[0:32, STEP_K:], [[(0, si)]], finish)


def send_edges(odd, u, h, x_msg, d_msg):
    for base, src in ((0, u), (3, h)):
        for c in range(3):
            low, top = src[every(2 * c), :], src[every(2 * c + 1), :]
            x_msg[base + c] = jnp.where(odd, top, low)
            d_msg[base + c] = jnp.where(odd, low, top)


def prep_body(
    count_ref, parity_ref, kmat_h, row_h, col_h, keep_h, u_h, scale_h, v_h, mass_h, ext_h,
    x_msg, d_msg, u_t, w_t, e_t, m_t, ei_t, si_t, a_out,
    kmat, row, col, keep, u_n, scale, v_n, mass, ext_n, h_t, sems,
):
    pairs = [
        (kmat_h, kmat), (row_h, row), (col_h, col), (keep_h, keep), (u_h, u_n),
        (scale_h, scale), (v_h, v_n), (mass_h, mass), (ext_h, ext_n),
    ]
    copies = [pltpu.make_async_copy(a, b, sems.at[n]) for n, (a, b) in enumerate(pairs)]
    for copy in copies:
        copy.start()
    for copy in copies:
        copy.wait()
    odd = parity_ref[0] == 1
    dt = step_size(count_ref)[0:1]
    high = lax.Precision.HIGHEST
    rows = jnp.dot(row[...], kmat[...], precision=high, preferred_element_type=F32)
    full = keep[0] * jnp.dot(rows, col[0], precision=high, preferred_element_type=F32)
    full = full + keep[1] * jnp.dot(rows, col[1], precision=high, preferred_element_type=F32)
    big = full.astype(jnp.bfloat16).astype(F32)
    slot = lax.broadcasted_iota(jnp.int32, full.shape, 1)
    main = (slot < 128) | ((slot >= STEP_K) & (slot < STEP_K + 64))
    a_out[...] = jnp.where(main, big, full - big).astype(jnp.bfloat16)
    inv = [(dt * dt) / mass[p] for p in range(2)]
    blank = jnp.zeros((ROWS, COLS), F32)
    for q in (6, 7):
        for ref in (u_t, w_t, e_t, m_t, si_t):
            ref[every(q), :] = blank
    for c in range(3):
        for p in range(2):
            q = 2 * c + p
            u_t[every(q), :] = u_n[q]
            w_t[every(q), :] = dt * v_n[q]
            e_t[every(q), :] = inv[p] * ext_n[q]
            m_t[every(q), :] = inv[p]
            si_t[every(q), :] = scale[0]
    inner_pass(a_out, si_t, e_t, m_t, u_t, w_t, ei_t, h_t)
    send_edges(odd, u_t, h_t, x_msg, d_msg)
    x_msg[6] = jnp.where(odd, inv[1], inv[0])
    d_msg[6] = jnp.where(odd, inv[0], inv[1])
    x_msg[7] = scale[1]
    d_msg[7] = scale[1]


def round_body(rnd, *refs):
    refs = list(refs)
    take = lambda n: [refs.pop(0) for _ in range(n)]
    count_ref, parity_ref = take(2)
    last = rnd == ROUNDS - 1
    if last:
        place_ref, own, peer, normal, before = take(5)
    x_in, d_in, u_t, w_t, e_t, m_t, ei_t, si_t, a_ref = take(9)
    if rnd == 0:
        (scale,) = take(1)
    else:
        sx_t, mh_t = take(2)
    if last:
        u_out, w2, g_out = take(3)
    else:
        x_msg, d_msg, u2, w2, ei_out = take(5)
    if rnd == 0:
        sx_t, mh_t = take(2)
    uh, hh, u1, u1h, w1, h_t = take(6)
    if last:
        u2, hits = take(2)
    odd = parity_ref[0] == 1

    def lower(k):
        return jnp.where(odd, d_in[k], x_in[k])

    def upper(k):
        return jnp.where(odd, x_in[k], d_in[k])

    blank = jnp.zeros((ROWS, COLS), F32)
    for q in (6, 7):
        for ref in (uh, hh) + ((mh_t, sx_t) if rnd == 0 else ()):
            ref[every(q), :] = blank
    act = [jnp.where(count_ref[0] > 2 * rnd + k, 1.0, 0.0).astype(F32) for k in range(2)]
    for c in range(3):
        for p, get in ((0, lower), (1, upper)):
            q = 2 * c + p
            uh[every(q), :] = get(c)
            hh[every(q), :] = get(3 + c)
            if rnd == 0:
                mh_t[every(q), :] = get(6)
                sx_t[every(q), :] = scale[1] if p else lower(7)

    def finish_first(n, r, force):
        at = tile(r)
        if n == 0:
            w = w_t[at, :] + act[0] * (ei_t[at, :] - m_t[at, :] * force)
            w1[at, :] = w
            u1[at, :] = u_t[at, :] + act[0] * w
        else:
            before = uh[at, :]
            u1h[at, :] = before + act[0] * ((hh[at, :] - mh_t[at, :] * force) - before)

    sweep(step_rows(u_t, uh), a_ref[32:96, 0:STEP_K], [[(0, sx_t)], [(32, sx_t)]], finish_first)

    def finish_second(n, r, force):
        at = tile(r)
        w = w1[at, :] + act[1] * (e_t[at, :] - m_t[at, :] * force)
        w2[at, :] = w
        u2[at, :] = u1[at, :] + act[1] * w

    sweep(step_rows(u1, u1h), a_ref[0:64, 0:STEP_K], [[(0, si_t), (32, sx_t)]], finish_second)
    if last:
        for q in range(6):
            u_out[q] = u2[every(q), :]
        partial_gaps(count_ref, place_ref, own, peer, normal, before, w2, g_out, hits)
        return
    inner_pass(a_ref, si_t, e_t, m_t, u2, w2, ei_out, h_t)
    send_edges(odd, u2, h_t, x_msg, d_msg)


def node_of(index):
    plane = index // (ROWS * COLS)
    row = (index // COLS) % ROWS
    return plane, pl.ds(pl.multiple_of(row * 8, 8), 8), index % COLS


def node_hits(plane, col):
    sub = lax.broadcasted_iota(jnp.int32, (8, COLS), 0)
    lane = lax.broadcasted_iota(jnp.int32, (8, COLS), 1)
    return [(sub == 2 * c + plane) & (lane == col) for c in range(3)]


def partial_gaps(count_ref, place_ref, own, peer, normal, before, w_in, g_out, hits):
    dt = step_size(count_ref)
    eighth = place_ref[0] % 8
    for side, nodes, vec, sign in ((0, own, normal, 1.0), (1, peer, before, -1.0)):
        for j in range(16):
            plane, at, col = node_of(nodes[j])
            value = w_in[at, :]
            total = jnp.zeros((8, COLS), F32)
            for c, hit in enumerate(node_hits(plane, col)):
                total = jnp.where(hit, value * vec[c, j], total)
            hits[side * 16 + j] = total
        total = jnp.sum(hits[side * 16 : side * 16 + 16], axis=1)
        total = jnp.sum(total, axis=1, keepdims=True) * (sign / dt[0:1, 0:1])
        lane = lax.broadcasted_iota(jnp.int32, (16, COLS), 1)
        sub = lax.broadcasted_iota(jnp.int32, (16, COLS), 0)
        line = jnp.where(lane == sub + 16 * eighth, jnp.broadcast_to(total, (16, COLS)), 0.0)
        line = jnp.sum(line, axis=0, keepdims=True)
        g_out[:, side * COLS : (side + 1) * COLS] = jnp.broadcast_to(line, (128, COLS))


def final_body(
    count_ref, own, peer, normal, before, gathered, inv_own, inv_before, w_in, m_own,
    v_out, work, mult,
):
    dt = step_size(count_ref)
    mine = jnp.sum(gathered[:, 0:COLS].reshape(16, 8, COLS), axis=1)
    other = jnp.sum(gathered[:, COLS : 2 * COLS].reshape(16, 8, COLS), axis=1)
    gap = mine + jnp.concatenate([other[4:16], other[0:4]], 0)
    for side, rows in ((0, inv_own), (1, inv_before)):
        acc = jnp.zeros((16, COLS), F32)
        for k in range(16):
            acc = acc + rows[:, k * COLS : (k + 1) * COLS] * gap[k : k + 1, :]
        lam = jnp.sum(acc, axis=1, keepdims=True)
        mult[side * 16 : side * 16 + 16, :] = jnp.broadcast_to(lam, (16, COLS))
    work[...] = w_in[...]
    for side, nodes, vec, sign in ((0, own, normal, -1.0), (1, peer, before, 1.0)):
        for j in range(16):
            plane, at, col = node_of(nodes[j])
            k = side * 16 + j
            value = work[at, :]
            change = m_own[at, :] * (mult[k : k + 1, :] * (sign / dt[0:1]))
            for c, hit in enumerate(node_hits(plane, col)):
                value = jnp.where(hit, value + change * vec[c, j], value)
            work[at, :] = value
    back = 1.0 / dt[0:1]
    for q in range(6):
        v_out[q] = work[every(q), :] * back


def call(body, outs, scratch, ins, limit=24 * 1024 * 1024):
    return pl.pallas_call(
        body,
        out_shape=[s if isinstance(s, jax.ShapeDtypeStruct) else jax.ShapeDtypeStruct(s, F32) for s in outs],
        in_specs=ins,
        out_specs=[VM] * len(outs),
        scratch_shapes=[pltpu.VMEM(s, F32) if isinstance(s, tuple) else s for s in scratch],
        compiler_params=pltpu.CompilerParams(vmem_limit_bytes=limit),
    )


TILE = (ROWS * 8, COLS)
PLANES = (6, ROWS, COLS)
WIDTH = STEP_K + INNER_K
ACROSS = [(i, i + 1) for i in range(1, 31, 2)] + [(i + 1, i) for i in range(1, 31, 2)]
WITHIN = [(i, i ^ 1) for i in range(32)]
FROM_BEFORE = [(i, (i + 1) % 4) for i in range(4)]


def on_device(
    displacement, velocity, external, mass, elem_scale, stiffness, substeps,
    own_nodes, peer_nodes, normals, schur_inverse,
):
    field = displacement[0].reshape(PLANES)
    speed = velocity[0].reshape(PLANES)
    loads = external[0].reshape(PLANES)
    weight = mass[0]
    scale = elem_scale[0]
    place = lax.axis_index("dom").reshape(1)
    parity = place % 2
    own = own_nodes[0]
    peer = peer_nodes[0]
    normal = normals[0]

    first = (8, ROWS, COLS)
    pair = (2, ROWS, COLS)
    weights = jax.ShapeDtypeStruct((96, WIDTH), jnp.bfloat16)
    x, d, u, w, e, m, ei, si, a = call(
        prep_body,
        [first, first, TILE, TILE, TILE, TILE, TILE, TILE, weights],
        [
            (24, 24), (96, 24), (2, 24, WIDTH), (2, 96, WIDTH), PLANES, pair, PLANES, pair, PLANES,
            TILE, pltpu.SemaphoreType.DMA((9,)),
        ],
        [SM] * 2 + [HBM] * 9,
    )(substeps, parity, stiffness[0], PICK_ROW, PICK_COL, KEEP, field, scale, speed, weight, loads)
    inv_before = before = None
    for rnd in range(ROUNDS):
        x = lax.ppermute(x, "dom", ACROSS)
        d = lax.ppermute(d, "dom", WITHIN)
        if rnd == 0:
            inv_before = lax.ppermute(schur_inverse, "grp", FROM_BEFORE)
            before = lax.ppermute(normal, "grp", FROM_BEFORE)
            x, d, inv_before, before = lax.optimization_barrier((x, d, inv_before, before))
        last = rnd == ROUNDS - 1
        args = [substeps, parity]
        if last:
            args += [place, own, peer, normal, before]
        scalars = len(args)
        args += [x, d, u, w, e, m, ei, si, a]
        args += [scale] if rnd == 0 else [sx, mh]
        outs = [PLANES, TILE, (128, 2 * COLS)] if last else [PLANES, PLANES, TILE, TILE, TILE]
        outs += [TILE, TILE] if rnd == 0 else []
        scratch = [TILE] * 6 + ([TILE, (32, 8, COLS)] if last else [])

        def body(*refs, rnd=rnd):
            return round_body(rnd, *refs)

        got = call(body, outs, scratch, [SM] * scalars + [VM] * (len(args) - scalars))(*args)
        if last:
            u, w, gap = got
        else:
            x, d, u, w, ei = got[:5]
        if rnd == 0:
            sx, mh = got[5:]
    gathered = lax.all_to_all(gap, ("grp", "dom"), 0, 0, tiled=True)
    (v,) = call(final_body, [PLANES], [TILE, (32, COLS)], [SM] * 5 + [VM] * 5)(
        substeps, own, peer, normal, before, gathered, schur_inverse, inv_before, w, m
    )
    shape = displacement.shape
    return u.reshape(shape), v.reshape(shape)


def solution(mesh):
    return jax.shard_map(
        on_device,
        mesh=mesh,
        in_specs=(
            P("grp", None, "dom", None, None),
            P("grp", None, "dom", None, None),
            P("grp", None, "dom", None, None),
            P("grp", "dom", None, None),
            P("grp", "dom", None, None),
            P("grp", None, None),
            P("grp"),
            P("grp", "dom"),
            P("grp", "dom"),
            P("grp", None, "dom"),
            P(("grp", "dom"), None),
        ),
        out_specs=(P("grp", None, "dom", None, None), P("grp", None, "dom", None, None)),
        check_vma=False,
    )
```

```python
import jax
import jax.numpy as jnp
import numpy as np
from jax import lax
from jax.experimental import pallas as pl
from jax.experimental.pallas import tpu as pltpu
from jax.sharding import PartitionSpec as P

MAXSUB = 8
ROUNDS = MAXSUB // 2
COARSE = 0.4
ROWS = 96
HALF = ROWS // 2
COLS = 128
STEP_K, INNER_K = 256, 128
F32 = jnp.float32
VM = pl.BlockSpec(memory_space=pltpu.VMEM)
SM = pl.BlockSpec(memory_space=pltpu.SMEM)
HBM = pl.BlockSpec(memory_space=pltpu.HBM)


def describe():
    cols = []
    for b, kinds in ((0, 4), (1, 4), (0, 2), (1, 2)):
        for kind in range(kinds):
            for q in range(16):
                x, comp = q % 2, (q % 8) // 2
                plane = x if q < 8 else (-1 if x == 0 else 2)
                cols.append((b, kind % 2, plane, comp) if q % 8 < 6 else None)
    cols += [None] * (STEP_K - len(cols))
    for kind in range(6):
        for q in range(16):
            cols.append((q // 8, kind % 2, q % 2, (q % 8) // 2) if q % 8 < 6 else None)
    return cols + [None] * (STEP_K + INNER_K - len(cols))


def selectors():
    cols = describe()
    pick_row = np.zeros((96, 24), np.float32)
    pick_col = np.zeros((2, 24, len(cols)), np.float32)
    keep = np.zeros((2, 96, len(cols)), np.float32)
    for k, slot in enumerate(cols):
        if slot is not None:
            b, e, plane, comp = slot
            for a in (0, 1):
                pick_col[a, (4 * a + 2 * b + e) * 3 + comp, k] = 1.0
    for block in range(3):
        for be in range(4):
            for q in range(6):
                comp, x = divmod(q, 2)
                layer = 0 if block == 0 else (-1 if x == 0 else 1)
                a = 1 - x if block == 1 else x
                m = block * 32 + be * 8 + q
                pick_row[m, (4 * a + be) * 3 + comp] = 1.0
                for k, slot in enumerate(cols):
                    if slot is not None and slot[2] - layer in (0, 1):
                        keep[slot[2] - layer, m, k] = 1.0
    return pick_row, pick_col, keep


PICK_ROW, PICK_COL, KEEP = selectors()


def step_size(count_ref):
    count = jnp.full((8, COLS), count_ref[0], jnp.int32).astype(F32)
    return COARSE / count


def lane_up(x):
    return pltpu.roll(x, COLS - 1, 1)


def lane_down(x):
    return pltpu.roll(x, 1, 1)


def every(i, stride=8):
    return pl.ds(i, ROWS, stride=stride)


def tile(r):
    return slice(8 * r, 8 * r + 8)


def split(u):
    hi = u.astype(jnp.bfloat16)
    lo = (u - hi.astype(F32)).astype(jnp.bfloat16)
    return [hi, lane_up(hi), lo, lane_up(lo)]


def step_rows(own, outer):
    done = {}

    def one(r):
        r %= ROWS
        if r not in done:
            done[r] = split(jnp.concatenate([own[tile(r), :], outer[tile(r), :]], 0))
        return done[r]

    def rows(r):
        here, there = one(r), one(r + 1)
        pad = jnp.zeros((64, COLS), jnp.bfloat16)
        return jnp.concatenate(here + there + here[:2] + there[:2] + [pad], 0)

    return rows


def inner_rows(own):
    def rows(r):
        parts = split(jnp.concatenate([own[tile(r), :], own[tile((r + 1) % ROWS), :]], 0))
        pad = jnp.zeros((32, COLS), jnp.bfloat16)
        return jnp.concatenate(parts + parts[:2] + [pad], 0)

    return rows


def sweep(rows, lhs, blocks, finish):
    carry = {}
    first = {}
    for i in range(HALF):
        rhs = jnp.concatenate([rows(i), rows(i + HALF)], 1)
        out = jnp.dot(lhs, rhs, preferred_element_type=F32)
        for h in range(2):
            r = i + h * HALF
            for n, terms in enumerate(blocks):
                part = []
                for b in range(2):
                    g = []
                    for e in range(2):
                        total = None
                        for offset, scale in terms:
                            j = offset + 16 * b + 8 * e
                            term = scale[tile(r), :] * out[j : j + 8, h * COLS : (h + 1) * COLS]
                            total = term if total is None else total + term
                        g.append(total)
                    part.append(g[0] + lane_down(g[1]))
                if i == 0:
                    first[h, n] = part[0]
                else:
                    finish(n, r, part[0] + carry[h, n])
                carry[h, n] = part[1]
    for n in range(len(blocks)):
        finish(n, 0, first[0, n] + carry[1, n])
        finish(n, HALF, first[1, n] + carry[0, n])


def inner_pass(a_ref, si, e, m, u, w, ei_out, h_out):
    def finish(n, r, force):
        at = tile(r)
        rest = e[at, :] - m[at, :] * force
        ei_out[at, :] = rest
        h_out[at, :] = u[at, :] + (w[at, :] + rest)

    sweep(inner_rows(u), a_ref[0:32, STEP_K:], [[(0, si)]], finish)


def send_edges(odd, u, h, x_msg, d_msg):
    for base, src in ((0, u), (3, h)):
        for c in range(3):
            low, top = src[every(2 * c), :], src[every(2 * c + 1), :]
            x_msg[base + c] = jnp.where(odd, top, low)
            d_msg[base + c] = jnp.where(odd, low, top)


def prep_body(
    count_ref, parity_ref, kmat_h, row_h, col_h, keep_h, u_h, scale_h, v_h, mass_h, ext_h,
    x_msg, d_msg, u_t, w_t, e_t, m_t, ei_t, si_t, a_out,
    kmat, row, col, keep, u_n, scale, v_n, mass, ext_n, h_t, sems,
):
    pairs = [
        (kmat_h, kmat), (row_h, row), (col_h, col), (keep_h, keep), (u_h, u_n),
        (scale_h, scale), (v_h, v_n), (mass_h, mass), (ext_h, ext_n),
    ]
    copies = [pltpu.make_async_copy(a, b, sems.at[n]) for n, (a, b) in enumerate(pairs)]
    for copy in copies:
        copy.start()
    for copy in copies:
        copy.wait()
    odd = parity_ref[0] == 1
    dt = step_size(count_ref)[0:1]
    high = lax.Precision.HIGHEST
    rows = jnp.dot(row[...], kmat[...], precision=high, preferred_element_type=F32)
    full = keep[0] * jnp.dot(rows, col[0], precision=high, preferred_element_type=F32)
    full = full + keep[1] * jnp.dot(rows, col[1], precision=high, preferred_element_type=F32)
    big = full.astype(jnp.bfloat16).astype(F32)
    slot = lax.broadcasted_iota(jnp.int32, full.shape, 1)
    main = (slot < 128) | ((slot >= STEP_K) & (slot < STEP_K + 64))
    a_out[...] = jnp.where(main, big, full - big).astype(jnp.bfloat16)
    inv = [(dt * dt) / mass[p] for p in range(2)]
    blank = jnp.zeros((ROWS, COLS), F32)
    for q in (6, 7):
        for ref in (u_t, w_t, e_t, m_t, si_t):
            ref[every(q), :] = blank
    for c in range(3):
        for p in range(2):
            q = 2 * c + p
            u_t[every(q), :] = u_n[q]
            w_t[every(q), :] = dt * v_n[q]
            e_t[every(q), :] = inv[p] * ext_n[q]
            m_t[every(q), :] = inv[p]
            si_t[every(q), :] = scale[0]
    inner_pass(a_out, si_t, e_t, m_t, u_t, w_t, ei_t, h_t)
    send_edges(odd, u_t, h_t, x_msg, d_msg)
    x_msg[6] = jnp.where(odd, inv[1], inv[0])
    d_msg[6] = jnp.where(odd, inv[0], inv[1])
    x_msg[7] = scale[1]
    d_msg[7] = scale[1]


def round_body(rnd, *refs):
    refs = list(refs)
    take = lambda n: [refs.pop(0) for _ in range(n)]
    count_ref, parity_ref = take(2)
    last = rnd == ROUNDS - 1
    if last:
        (place_ref,) = take(1)
    x_in, d_in, u_t, w_t, e_t, m_t, ei_t, si_t, a_ref = take(9)
    if rnd == 0:
        (scale,) = take(1)
    else:
        sx_t, mh_t = take(2)
    if last:
        pick, share = take(2)
        u_out, v_out, g_out = take(3)
    else:
        x_msg, d_msg, u2, w2, ei_out = take(5)
    if rnd == 0:
        sx_t, mh_t = take(2)
    uh, hh, u1, u1h, w1, h_t = take(6)
    if last:
        u2, w2 = take(2)
    odd = parity_ref[0] == 1

    def lower(k):
        return jnp.where(odd, d_in[k], x_in[k])

    def upper(k):
        return jnp.where(odd, x_in[k], d_in[k])

    blank = jnp.zeros((ROWS, COLS), F32)
    for q in (6, 7):
        for ref in (uh, hh) + ((mh_t, sx_t) if rnd == 0 else ()):
            ref[every(q), :] = blank
    act = [jnp.where(count_ref[0] > 2 * rnd + k, 1.0, 0.0).astype(F32) for k in range(2)]
    for c in range(3):
        for p, get in ((0, lower), (1, upper)):
            q = 2 * c + p
            uh[every(q), :] = get(c)
            hh[every(q), :] = get(3 + c)
            if rnd == 0:
                mh_t[every(q), :] = get(6)
                sx_t[every(q), :] = scale[1] if p else lower(7)

    def finish_first(n, r, force):
        at = tile(r)
        if n == 0:
            w = w_t[at, :] + act[0] * (ei_t[at, :] - m_t[at, :] * force)
            w1[at, :] = w
            u1[at, :] = u_t[at, :] + act[0] * w
        else:
            before = uh[at, :]
            u1h[at, :] = before + act[0] * ((hh[at, :] - mh_t[at, :] * force) - before)

    sweep(step_rows(u_t, uh), a_ref[32:96, 0:STEP_K], [[(0, sx_t)], [(32, sx_t)]], finish_first)

    def finish_second(n, r, force):
        at = tile(r)
        w = w1[at, :] + act[1] * (e_t[at, :] - m_t[at, :] * force)
        w2[at, :] = w
        u2[at, :] = u1[at, :] + act[1] * w

    sweep(step_rows(u1, u1h), a_ref[0:64, 0:STEP_K], [[(0, si_t), (32, sx_t)]], finish_second)
    if last:
        for q in range(6):
            u_out[q] = u2[every(q), :]
            v_out[q] = w2[every(q), :] / step_size(count_ref)[0:1]
        partial_gaps(place_ref, pick, share, v_out, g_out)
        return
    inner_pass(a_ref, si_t, e_t, m_t, u2, w2, ei_out, h_t)
    send_edges(odd, u2, h_t, x_msg, d_msg)


def thirds(x):
    parts = []
    for _ in range(3):
        part = x.astype(jnp.bfloat16)
        parts.append(part)
        x = x - part.astype(F32)
    return parts


def chosen(onehot, values):
    return sum(jnp.dot(onehot, part, preferred_element_type=F32) for part in thirds(values))


def node_body(own, peer, normal, before, mass, pick, pick_t, share, change):
    sub = lax.broadcasted_iota(jnp.int32, (16, 16), 0)
    eye = sub == lax.broadcasted_iota(jnp.int32, (16, 16), 1)
    lane = lax.broadcasted_iota(jnp.int32, (16, COLS), 1)
    weights = jnp.concatenate([mass[0], mass[1]], 1)

    def column(line):
        return jnp.sum(jnp.where(eye, jnp.broadcast_to(line, (16, 16)), 0.0), axis=1, keepdims=True)

    for side, nodes, vec, sign in ((0, own, normal, 1.0), (1, peer, before, -1.0)):
        at = slice(16 * side, 16 * side + 16)
        index = column(nodes[...].astype(F32)).astype(jnp.int32)
        plane = jnp.where(index >= ROWS * COLS, 1, 0)
        rest = index - plane * (ROWS * COLS)
        row = rest // COLS
        col = rest - row * COLS
        onehot = jnp.where(lane == row, 1.0, 0.0)
        pick[at, :] = onehot[:, 0:ROWS].astype(jnp.bfloat16)
        heavy = chosen(onehot[:, 0:ROWS].astype(jnp.bfloat16), weights)
        hits = [(lane == col) & (plane == p) for p in range(2)]
        total = jnp.where(hits[0], heavy[:, 0:COLS], 0.0) + jnp.where(hits[1], heavy[:, COLS:], 0.0)
        total = jnp.sum(total, axis=1, keepdims=True)
        for c in range(3):
            value = sign * column(vec[c : c + 1, :])
            for p in range(2):
                q = 2 * c + p
                part = jnp.where(hits[p], value, 0.0)
                share[at, q * COLS : (q + 1) * COLS] = part
                change[at, q * COLS : (q + 1) * COLS] = -part / total
        pick_t[side] = jnp.transpose(onehot)[0:ROWS].astype(jnp.bfloat16)


def partial_gaps(place_ref, pick, share, v, g_out):
    values = jnp.concatenate([v[q] for q in range(6)], 1)
    total = jnp.sum(chosen(pick[...], values) * share[...], axis=1, keepdims=True)
    lane = lax.broadcasted_iota(jnp.int32, (32, COLS), 1)
    sub = lax.broadcasted_iota(jnp.int32, (32, COLS), 0)
    line = jnp.where(lane == sub % 16 + 16 * (place_ref[0] % 8), jnp.broadcast_to(total, (32, COLS)), 0.0)
    for side in range(2):
        part = jnp.sum(line[16 * side : 16 * side + 16], axis=0, keepdims=True)
        g_out[:, side * COLS : (side + 1) * COLS] = jnp.broadcast_to(part, (128, COLS))


def final_body(gathered, inv_own, inv_before, pick_t, change, v_in, v_out):
    mine = jnp.sum(gathered[:, 0:COLS].reshape(16, 8, COLS), axis=1)
    other = jnp.sum(gathered[:, COLS : 2 * COLS].reshape(16, 8, COLS), axis=1)
    gap = mine + jnp.concatenate([other[4:16], other[0:4]], 0)
    total = None
    for side, rows in ((0, inv_own), (1, inv_before)):
        acc = jnp.zeros((16, COLS), F32)
        for k in range(16):
            acc = acc + rows[:, k * COLS : (k + 1) * COLS] * gap[k : k + 1, :]
        lam = jnp.sum(acc, axis=1, keepdims=True)
        part = chosen(pick_t[side], change[16 * side : 16 * side + 16, :] * lam)
        total = part if total is None else total + part
    for q in range(6):
        v_out[q] = v_in[q] + total[:, q * COLS : (q + 1) * COLS]


def call(body, outs, scratch, ins, limit=24 * 1024 * 1024):
    return pl.pallas_call(
        body,
        out_shape=[s if isinstance(s, jax.ShapeDtypeStruct) else jax.ShapeDtypeStruct(s, F32) for s in outs],
        in_specs=ins,
        out_specs=[VM] * len(outs),
        scratch_shapes=[pltpu.VMEM(s, F32) if isinstance(s, tuple) else s for s in scratch],
        compiler_params=pltpu.CompilerParams(vmem_limit_bytes=limit),
    )


TILE = (ROWS * 8, COLS)
PLANES = (6, ROWS, COLS)
WIDTH = STEP_K + INNER_K
ACROSS = [(i, i + 1) for i in range(1, 31, 2)] + [(i + 1, i) for i in range(1, 31, 2)]
WITHIN = [(i, i ^ 1) for i in range(32)]
FROM_BEFORE = [(i, (i + 1) % 4) for i in range(4)]


def far(x):
    return pltpu.with_memory_space_constraint(jnp.asarray(x), pltpu.HBM)


def on_device(
    displacement, velocity, external, mass, elem_scale, stiffness, substeps,
    own_nodes, peer_nodes, normals, schur_inverse,
):
    field = displacement[0].reshape(PLANES)
    speed = velocity[0].reshape(PLANES)
    loads = external[0].reshape(PLANES)
    weight = mass[0]
    scale = elem_scale[0]
    place = lax.axis_index("dom").reshape(1)
    parity = place % 2
    normal = normals[0]

    first = (8, ROWS, COLS)
    pair = (2, ROWS, COLS)
    weights = jax.ShapeDtypeStruct((96, WIDTH), jnp.bfloat16)
    x, d, u, w, e, m, ei, si, a = call(
        prep_body,
        [first, first, TILE, TILE, TILE, TILE, TILE, TILE, weights],
        [
            (24, 24), (96, 24), (2, 24, WIDTH), (2, 96, WIDTH), PLANES, pair, PLANES, pair, PLANES,
            TILE, pltpu.SemaphoreType.DMA((9,)),
        ],
        [SM] * 2 + [HBM] * 9,
    )(substeps, parity, *(far(v) for v in (stiffness[0], PICK_ROW, PICK_COL, KEEP, field, scale, speed, weight, loads)))
    inv_before = before = None
    for rnd in range(ROUNDS):
        x = lax.ppermute(x, "dom", ACROSS)
        d = lax.ppermute(d, "dom", WITHIN)
        if rnd == 0:
            inv_before = lax.ppermute(schur_inverse, "grp", FROM_BEFORE)
            before = lax.ppermute(normal, "grp", FROM_BEFORE)
            x, d, inv_before, before = lax.optimization_barrier((x, d, inv_before, before))
        if rnd == 1:
            b16 = lambda *shape: jax.ShapeDtypeStruct(shape, jnp.bfloat16)
            nodes = call(
                node_body, [b16(32, ROWS), b16(2, ROWS, 16), (32, 6 * COLS), (32, 6 * COLS)], [], [VM] * 5
            )(own_nodes, peer_nodes, normal, before, weight)
            x, d, *nodes = lax.optimization_barrier((x, d, *nodes))
            pick, pick_t, share, change = nodes
        last = rnd == ROUNDS - 1
        args = [substeps, parity]
        if last:
            args += [place]
        scalars = len(args)
        args += [x, d, u, w, e, m, ei, si, a]
        args += [scale] if rnd == 0 else [sx, mh]
        args += [pick, share] if last else []
        outs = [PLANES, PLANES, (128, 2 * COLS)] if last else [PLANES, PLANES, TILE, TILE, TILE]
        outs += [TILE, TILE] if rnd == 0 else []
        scratch = [TILE] * (8 if last else 6)

        def body(*refs, rnd=rnd):
            return round_body(rnd, *refs)

        got = call(body, outs, scratch, [SM] * scalars + [VM] * (len(args) - scalars))(*args)
        if last:
            u, v, gap = got
        else:
            x, d, u, w, ei = got[:5]
        if rnd == 0:
            sx, mh = got[5:]
    gathered = lax.all_to_all(gap, ("grp", "dom"), 0, 0, tiled=True)
    (v,) = call(final_body, [PLANES], [], [VM] * 6)(
        gathered, schur_inverse, inv_before, pick_t, change, v
    )
    shape = displacement.shape
    return u.reshape(shape), v.reshape(shape)


def solution(mesh):
    return jax.shard_map(
        on_device,
        mesh=mesh,
        in_specs=(
            P("grp", None, "dom", None, None),
            P("grp", None, "dom", None, None),
            P("grp", None, "dom", None, None),
            P("grp", "dom", None, None),
            P("grp", "dom", None, None),
            P("grp", None, None),
            P("grp"),
            P("grp", "dom"),
            P("grp", "dom"),
            P("grp", None, "dom"),
            P(("grp", "dom"), None),
        ),
        out_specs=(P("grp", None, "dom", None, None), P("grp", None, "dom", None, None)),
        check_vma=False,
    )
```

```python
import jax
import jax.numpy as jnp
import numpy as np
from jax import lax
from jax.experimental import pallas as pl
from jax.experimental.pallas import tpu as pltpu
from jax.sharding import PartitionSpec as P

MAXSUB = 8
ROUNDS = MAXSUB // 2
GROUPS = 4
DOMS = 32
COARSE = 0.4
ROWS = 96
HALF = ROWS // 2
COLS = 128
STEP_K, INNER_K = 256, 128
F32 = jnp.float32
VM = pl.BlockSpec(memory_space=pltpu.VMEM)
SM = pl.BlockSpec(memory_space=pltpu.SMEM)
HBM = pl.BlockSpec(memory_space=pltpu.HBM)


def describe():
    cols = []
    for b, kinds in ((0, 4), (1, 4), (0, 2), (1, 2)):
        for kind in range(kinds):
            for q in range(16):
                x, comp = q % 2, (q % 8) // 2
                plane = x if q < 8 else (-1 if x == 0 else 2)
                cols.append((b, kind % 2, plane, comp) if q % 8 < 6 else None)
    cols += [None] * (STEP_K - len(cols))
    for kind in range(6):
        for q in range(16):
            cols.append((q // 8, kind % 2, q % 2, (q % 8) // 2) if q % 8 < 6 else None)
    return cols + [None] * (STEP_K + INNER_K - len(cols))


def selectors():
    cols = describe()
    pick_row = np.zeros((96, 24), np.float32)
    pick_col = np.zeros((2, 24, len(cols)), np.float32)
    keep = np.zeros((2, 96, len(cols)), np.float32)
    for k, slot in enumerate(cols):
        if slot is not None:
            b, e, plane, comp = slot
            for a in (0, 1):
                pick_col[a, (4 * a + 2 * b + e) * 3 + comp, k] = 1.0
    for block in range(3):
        for be in range(4):
            for q in range(6):
                comp, x = divmod(q, 2)
                layer = 0 if block == 0 else (-1 if x == 0 else 1)
                a = 1 - x if block == 1 else x
                m = block * 32 + be * 8 + q
                pick_row[m, (4 * a + be) * 3 + comp] = 1.0
                for k, slot in enumerate(cols):
                    if slot is not None and slot[2] - layer in (0, 1):
                        keep[slot[2] - layer, m, k] = 1.0
    return pick_row, pick_col, keep


PICK_ROW, PICK_COL, KEEP = selectors()


def step_size(count_ref):
    count = jnp.full((8, COLS), count_ref[0], jnp.int32).astype(F32)
    return COARSE / count


def lane_up(x):
    return pltpu.roll(x, COLS - 1, 1)


def lane_down(x):
    return pltpu.roll(x, 1, 1)


def every(i, stride=8):
    return pl.ds(i, ROWS, stride=stride)


def tile(r):
    return slice(8 * r, 8 * r + 8)


def split(u):
    hi = u.astype(jnp.bfloat16)
    lo = (u - hi.astype(F32)).astype(jnp.bfloat16)
    return [hi, lane_up(hi), lo, lane_up(lo)]


def step_rows(own, outer):
    done = {}

    def one(r):
        r %= ROWS
        if r not in done:
            done[r] = split(jnp.concatenate([own[tile(r), :], outer[tile(r), :]], 0))
        return done[r]

    def rows(r):
        here, there = one(r), one(r + 1)
        pad = jnp.zeros((64, COLS), jnp.bfloat16)
        return jnp.concatenate(here + there + here[:2] + there[:2] + [pad], 0)

    return rows


def inner_rows(own):
    def rows(r):
        here, there = tile(r % ROWS), tile((r + 1) % ROWS)
        parts = split(jnp.concatenate([own[here, :], own[there, :]], 0))
        pad = jnp.zeros((32, COLS), jnp.bfloat16)
        return jnp.concatenate(parts + parts[:2] + [pad], 0)

    return rows


def sweep(start, rows, lhs, blocks, finish):
    carry = {}
    first = {}
    for i in range(start, start + HALF):
        rhs = jnp.concatenate([rows(i), rows(i + HALF)], 1)
        out = jnp.dot(lhs, rhs, preferred_element_type=F32)
        for h in range(2):
            r = (i + h * HALF) % ROWS
            for n, terms in enumerate(blocks):
                part = []
                for b in range(2):
                    g = []
                    for e in range(2):
                        total = None
                        for offset, scale in terms:
                            j = offset + 16 * b + 8 * e
                            term = scale[tile(r), :] * out[j : j + 8, h * COLS : (h + 1) * COLS]
                            total = term if total is None else total + term
                        g.append(total)
                    part.append(g[0] + lane_down(g[1]))
                if i == start:
                    first[h, n] = part[0]
                else:
                    finish(n, r, part[0] + carry[h, n])
                carry[h, n] = part[1]
    for n in range(len(blocks)):
        finish(n, start, first[0, n] + carry[1, n])
        finish(n, start + HALF, first[1, n] + carry[0, n])


def inner_pass(a_ref, si, e, m, u, w, ei_out, h_out):
    def finish(n, r, force):
        at = tile(r)
        rest = e[at, :] - m[at, :] * force
        ei_out[at, :] = rest
        h_out[at, :] = u[at, :] + (w[at, :] + rest)

    sweep(2, inner_rows(u), a_ref[0:32, STEP_K:], [[(0, si)]], finish)


def send_edges(odd, u, h, x_msg, d_msg):
    for base, src in ((0, u), (3, h)):
        for c in range(3):
            low, top = src[every(2 * c), :], src[every(2 * c + 1), :]
            x_msg[base + c] = jnp.where(odd, top, low)
            d_msg[base + c] = jnp.where(odd, low, top)


def prep_body(
    count_ref, place_ref, kmat_h, row_h, col_h, keep_h, u_h, scale_h, v_h, mass_h, ext_h,
    x_msg, d_msg, u_t, w_t, e_t, m_t, ei_t, si_t, a_out,
    kmat, row, col, keep, u_n, scale, v_n, mass, ext_n, h_t, sems,
):
    pairs = [
        (kmat_h, kmat), (row_h, row), (col_h, col), (keep_h, keep), (u_h, u_n),
        (scale_h, scale), (v_h, v_n), (mass_h, mass), (ext_h, ext_n),
    ]
    copies = [pltpu.make_async_copy(a, b, sems.at[n]) for n, (a, b) in enumerate(pairs)]
    for copy in copies:
        copy.start()
    for copy in copies:
        copy.wait()
    odd = place_ref[0] % 2 == 1
    dt = step_size(count_ref)[0:1]
    high = lax.Precision.HIGHEST
    rows = jnp.dot(row[...], kmat[...], precision=high, preferred_element_type=F32)
    full = keep[0] * jnp.dot(rows, col[0], precision=high, preferred_element_type=F32)
    full = full + keep[1] * jnp.dot(rows, col[1], precision=high, preferred_element_type=F32)
    big = full.astype(jnp.bfloat16).astype(F32)
    slot = lax.broadcasted_iota(jnp.int32, full.shape, 1)
    main = (slot < 128) | ((slot >= STEP_K) & (slot < STEP_K + 64))
    a_out[...] = jnp.where(main, big, full - big).astype(jnp.bfloat16)
    inv = [(dt * dt) / mass[p] for p in range(2)]
    blank = jnp.zeros((ROWS, COLS), F32)
    for q in (6, 7):
        for ref in (u_t, w_t, e_t, m_t, si_t):
            ref[every(q), :] = blank
    for c in range(3):
        for p in range(2):
            q = 2 * c + p
            u_t[every(q), :] = u_n[q]
            w_t[every(q), :] = dt * v_n[q]
            e_t[every(q), :] = inv[p] * ext_n[q]
            m_t[every(q), :] = inv[p]
            si_t[every(q), :] = scale[0]
    inner_pass(a_out, si_t, e_t, m_t, u_t, w_t, ei_t, h_t)
    send_edges(odd, u_t, h_t, x_msg, d_msg)
    x_msg[6] = jnp.where(odd, inv[1], inv[0])
    d_msg[6] = jnp.where(odd, inv[0], inv[1])
    x_msg[7] = scale[1]
    d_msg[7] = scale[1]


def round_body(rnd, *refs):
    refs = list(refs)
    take = lambda n: [refs.pop(0) for _ in range(n)]
    count_ref, place_ref = take(2)
    last = rnd == ROUNDS - 1
    x_in, d_in, u_t, w_t, e_t, m_t, ei_t, si_t, a_ref = take(9)
    if rnd == 0:
        (scale,) = take(1)
    else:
        sx_t, mh_t = take(2)
    if last:
        pick, share = take(2)
        u_out, v_out, g_out = take(3)
    else:
        x_msg, d_msg, u2, w2, ei_out = take(5)
    if rnd == 0:
        sx_t, mh_t = take(2)
    uh, hh, u1, u1h, w1, h_t = take(6)
    if last:
        u2, w2 = take(2)
    place = place_ref[0]
    odd = place % 2 == 1
    inside = (place > 0) & (place < DOMS - 1)

    def across(k):
        return jnp.where(inside, x_in[k], 0.0)

    def lower(k):
        return jnp.where(odd, d_in[k], across(k))

    def upper(k):
        return jnp.where(odd, across(k), d_in[k])

    blank = jnp.zeros((ROWS, COLS), F32)
    for q in (6, 7):
        for ref in (uh, hh) + ((mh_t, sx_t) if rnd == 0 else ()):
            ref[every(q), :] = blank
    act = [jnp.where(count_ref[0] > 2 * rnd + k, 1.0, 0.0).astype(F32) for k in range(2)]
    for c in range(3):
        for p, get in ((0, lower), (1, upper)):
            q = 2 * c + p
            uh[every(q), :] = get(c)
            hh[every(q), :] = get(3 + c)
            if rnd == 0:
                mh_t[every(q), :] = get(6)
                sx_t[every(q), :] = scale[1] if p else lower(7)

    def finish_first(n, r, force):
        at = tile(r)
        if n == 0:
            w = w_t[at, :] + act[0] * (ei_t[at, :] - m_t[at, :] * force)
            w1[at, :] = w
            u1[at, :] = u_t[at, :] + act[0] * w
        else:
            before = uh[at, :]
            u1h[at, :] = before + act[0] * ((hh[at, :] - mh_t[at, :] * force) - before)

    sweep(0, step_rows(u_t, uh), a_ref[32:96, 0:STEP_K], [[(0, sx_t)], [(32, sx_t)]], finish_first)

    def finish_second(n, r, force):
        at = tile(r)
        w = w1[at, :] + act[1] * (e_t[at, :] - m_t[at, :] * force)
        w2[at, :] = w
        u2[at, :] = u1[at, :] + act[1] * w

    sweep(1, step_rows(u1, u1h), a_ref[0:64, 0:STEP_K], [[(0, si_t), (32, sx_t)]], finish_second)
    if last:
        for q in range(6):
            u_out[q] = u2[every(q), :]
            v_out[q] = w2[every(q), :] / step_size(count_ref)[0:1]
        partial_gaps(place_ref, pick, share, v_out, g_out)
        return
    inner_pass(a_ref, si_t, e_t, m_t, u2, w2, ei_out, h_t)
    send_edges(odd, u2, h_t, x_msg, d_msg)


def thirds(x):
    parts = []
    for _ in range(3):
        part = x.astype(jnp.bfloat16)
        parts.append(part)
        x = x - part.astype(F32)
    return parts


def chosen(onehot, values):
    return sum(jnp.dot(onehot, part, preferred_element_type=F32) for part in thirds(values))


def node_body(own, peer, normal, before, mass, pick, pick_t, share, change):
    sub = lax.broadcasted_iota(jnp.int32, (16, 16), 0)
    eye = sub == lax.broadcasted_iota(jnp.int32, (16, 16), 1)
    lane = lax.broadcasted_iota(jnp.int32, (16, COLS), 1)
    weights = jnp.concatenate([mass[0], mass[1]], 1)

    def column(line):
        return jnp.sum(jnp.where(eye, jnp.broadcast_to(line, (16, 16)), 0.0), axis=1, keepdims=True)

    for side, nodes, vec, sign in ((0, own, normal, 1.0), (1, peer, before, -1.0)):
        at = slice(16 * side, 16 * side + 16)
        index = column(nodes[...].astype(F32)).astype(jnp.int32)
        plane = jnp.where(index >= ROWS * COLS, 1, 0)
        rest = index - plane * (ROWS * COLS)
        row = rest // COLS
        col = rest - row * COLS
        onehot = jnp.where(lane == row, 1.0, 0.0)
        pick[at, :] = onehot[:, 0:ROWS].astype(jnp.bfloat16)
        heavy = chosen(onehot[:, 0:ROWS].astype(jnp.bfloat16), weights)
        hits = [(lane == col) & (plane == p) for p in range(2)]
        total = jnp.where(hits[0], heavy[:, 0:COLS], 0.0) + jnp.where(hits[1], heavy[:, COLS:], 0.0)
        total = jnp.sum(total, axis=1, keepdims=True)
        for c in range(3):
            value = sign * column(vec[c : c + 1, :])
            for p in range(2):
                q = 2 * c + p
                part = jnp.where(hits[p], value, 0.0)
                share[at, q * COLS : (q + 1) * COLS] = part
                change[at, q * COLS : (q + 1) * COLS] = -part / total
        pick_t[side] = jnp.transpose(onehot)[0:ROWS].astype(jnp.bfloat16)


def partial_gaps(place_ref, pick, share, v, g_out):
    values = jnp.concatenate([v[q] for q in range(6)], 1)
    total = jnp.sum(chosen(pick[...], values) * share[...], axis=1, keepdims=True)
    lane = lax.broadcasted_iota(jnp.int32, (32, COLS), 1)
    sub = lax.broadcasted_iota(jnp.int32, (32, COLS), 0)
    line = jnp.where(lane == sub % 16 + 16 * (place_ref[0] % 8), jnp.broadcast_to(total, (32, COLS)), 0.0)
    for side in range(2):
        part = jnp.sum(line[16 * side : 16 * side + 16], axis=0, keepdims=True)
        g_out[:, side * COLS : (side + 1) * COLS] = jnp.broadcast_to(part, (128, COLS))


def final_body(gathered, inv_own, inv_before, pick_t, change, v_in, v_out):
    mine = jnp.sum(gathered[:, 0:COLS].reshape(16, 8, COLS), axis=1)
    other = jnp.sum(gathered[:, COLS : 2 * COLS].reshape(16, 8, COLS), axis=1)
    gap = mine + jnp.concatenate([other[4:16], other[0:4]], 0)
    total = None
    for side, rows in ((0, inv_own), (1, inv_before)):
        acc = jnp.zeros((16, COLS), F32)
        for k in range(16):
            acc = acc + rows[:, k * COLS : (k + 1) * COLS] * gap[k : k + 1, :]
        lam = jnp.sum(acc, axis=1, keepdims=True)
        part = chosen(pick_t[side], change[16 * side : 16 * side + 16, :] * lam)
        total = part if total is None else total + part
    for q in range(6):
        v_out[q] = v_in[q] + total[:, q * COLS : (q + 1) * COLS]


def call(body, outs, scratch, ins, limit=24 * 1024 * 1024):
    return pl.pallas_call(
        body,
        out_shape=[s if isinstance(s, jax.ShapeDtypeStruct) else jax.ShapeDtypeStruct(s, F32) for s in outs],
        in_specs=ins,
        out_specs=[VM] * len(outs),
        scratch_shapes=[pltpu.VMEM(s, F32) if isinstance(s, tuple) else s for s in scratch],
        compiler_params=pltpu.CompilerParams(vmem_limit_bytes=limit),
    )


TILE = (ROWS * 8, COLS)
PLANES = (6, ROWS, COLS)
WIDTH = STEP_K + INNER_K


def across_pairs():
    pairs = [(g * DOMS + i, g * DOMS + i + 1) for g in range(GROUPS) for i in range(1, DOMS - 1, 2)]
    for g in range(0, GROUPS, 2):
        for i in (0, DOMS - 1):
            pairs.append((g * DOMS + i, (g + 1) * DOMS + i))
    return pairs + [(b, a) for a, b in pairs]


ACROSS = across_pairs()
WITHIN = [(i, i ^ 1) for i in range(32)]
FROM_BEFORE = [(i, (i + 1) % 4) for i in range(4)]


def far(x):
    return pltpu.with_memory_space_constraint(jnp.asarray(x), pltpu.HBM)


def on_device(
    displacement, velocity, external, mass, elem_scale, stiffness, substeps,
    own_nodes, peer_nodes, normals, schur_inverse,
):
    field = displacement[0].reshape(PLANES)
    speed = velocity[0].reshape(PLANES)
    loads = external[0].reshape(PLANES)
    weight = mass[0]
    scale = elem_scale[0]
    place = lax.axis_index("dom").reshape(1)
    normal = normals[0]

    first = (8, ROWS, COLS)
    pair = (2, ROWS, COLS)
    weights = jax.ShapeDtypeStruct((96, WIDTH), jnp.bfloat16)
    x, d, u, w, e, m, ei, si, a = call(
        prep_body,
        [first, first, TILE, TILE, TILE, TILE, TILE, TILE, weights],
        [
            (24, 24), (96, 24), (2, 24, WIDTH), (2, 96, WIDTH), PLANES, pair, PLANES, pair, PLANES,
            TILE, pltpu.SemaphoreType.DMA((9,)),
        ],
        [SM] * 2 + [HBM] * 9,
    )(substeps, place, *(far(v) for v in (stiffness[0], PICK_ROW, PICK_COL, KEEP, field, scale, speed, weight, loads)))
    inv_before = before = None
    for rnd in range(ROUNDS):
        x = lax.ppermute(x, ("grp", "dom"), ACROSS)
        d = lax.ppermute(d, "dom", WITHIN)
        if rnd == 0:
            inv_before = lax.ppermute(schur_inverse, "grp", FROM_BEFORE)
            before = lax.ppermute(normal, "grp", FROM_BEFORE)
            x, d, inv_before, before = lax.optimization_barrier((x, d, inv_before, before))
        if rnd == 1:
            b16 = lambda *shape: jax.ShapeDtypeStruct(shape, jnp.bfloat16)
            nodes = call(
                node_body, [b16(32, ROWS), b16(2, ROWS, 16), (32, 6 * COLS), (32, 6 * COLS)], [], [VM] * 5
            )(own_nodes, peer_nodes, normal, before, weight)
            x, d, *nodes = lax.optimization_barrier((x, d, *nodes))
            pick, pick_t, share, change = nodes
        last = rnd == ROUNDS - 1
        args = [substeps, place]
        scalars = len(args)
        args += [x, d, u, w, e, m, ei, si, a]
        args += [scale] if rnd == 0 else [sx, mh]
        args += [pick, share] if last else []
        outs = [PLANES, PLANES, (128, 2 * COLS)] if last else [PLANES, PLANES, TILE, TILE, TILE]
        outs += [TILE, TILE] if rnd == 0 else []
        scratch = [TILE] * (8 if last else 6)

        def body(*refs, rnd=rnd):
            return round_body(rnd, *refs)

        got = call(body, outs, scratch, [SM] * scalars + [VM] * (len(args) - scalars))(*args)
        if last:
            u, v, gap = got
        else:
            x, d, u, w, ei = got[:5]
        if rnd == 0:
            sx, mh = got[5:]
    gathered = lax.all_to_all(gap, ("grp", "dom"), 0, 0, tiled=True)
    (v,) = call(final_body, [PLANES], [], [VM] * 6)(
        gathered, schur_inverse, inv_before, pick_t, change, v
    )
    shape = displacement.shape
    return u.reshape(shape), v.reshape(shape)


def solution(mesh):
    return jax.shard_map(
        on_device,
        mesh=mesh,
        in_specs=(
            P("grp", None, "dom", None, None),
            P("grp", None, "dom", None, None),
            P("grp", None, "dom", None, None),
            P("grp", "dom", None, None),
            P("grp", "dom", None, None),
            P("grp", None, None),
            P("grp"),
            P("grp", "dom"),
            P("grp", "dom"),
            P("grp", None, "dom"),
            P(("grp", "dom"), None),
        ),
        out_specs=(P("grp", None, "dom", None, None), P("grp", None, "dom", None, None)),
        check_vma=False,
    )
```

```python
import jax
import jax.numpy as jnp
import numpy as np
from jax import lax
from jax.experimental import pallas as pl
from jax.experimental.pallas import tpu as pltpu
from jax.sharding import PartitionSpec as P

MAXSUB = 8
ROUNDS = MAXSUB // 2
GROUPS = 4
DOMS = 32
COARSE = 0.4
ROWS = 96
HALF = ROWS // 2
COLS = 128
WIDTH = 256
F32 = jnp.float32
BF16 = jnp.bfloat16
VM = pl.BlockSpec(memory_space=pltpu.VMEM)
SM = pl.BlockSpec(memory_space=pltpu.SMEM)
HBM = pl.BlockSpec(memory_space=pltpu.HBM)


def describe():
    cols = []
    for low, kinds in ((0, 4), (1, 2)):
        for kind in range(kinds):
            for q in range(16):
                cols.append((q // 8, kind % 2, q % 8, low))
    for low in (0, 0, 1):
        for q in range(16):
            cols.append((2, q // 8, q % 8, low))
    return cols


def selectors():
    pick_row = np.zeros((2, 32, 24), np.float32)
    pick_col = np.zeros((2, 2, 24, WIDTH), np.float32)
    for w in range(2):
        for be in range(4):
            for q in range(6):
                pick_row[w, be * 8 + q, (4 * (q % 2 ^ w) + be) * 3 + q // 2] = 1.0
        for t in range(2):
            for k, (at, e, q, _) in enumerate(describe()):
                if q < 6 and at - t in (0, 1):
                    pick_col[w, t, (4 * (q % 2 ^ w) + 2 * (at - t) + e) * 3 + q // 2, k] = 1.0
    return pick_row, pick_col


PICK_ROW, PICK_COL = selectors()


def step_size(count_ref):
    count = jnp.full((8, COLS), count_ref[0], jnp.int32).astype(F32)
    return COARSE / count


def lane_up(x):
    return pltpu.roll(x, COLS - 1, 1)


def lane_down(x):
    return pltpu.roll(x, 1, 1)


def every(i, stride=8):
    return pl.ds(i, ROWS, stride=stride)


def tile(r):
    return slice(8 * (r % ROWS), 8 * (r % ROWS) + 8)


def halves(u):
    hi = u.astype(BF16)
    return hi, (u - hi.astype(F32)).astype(BF16)


def tile_rows(get):
    def rows(r):
        hi, lo = halves(jnp.concatenate([get(r), get(r + 1)], 0))
        parts = [hi, lane_up(hi), lo, lane_up(lo)]
        third = get(r + 2)
        hi, lo = halves(jnp.concatenate([third, lane_up(third)], 0))
        pad = jnp.zeros((WIDTH - 144, COLS), BF16)
        return jnp.concatenate(parts + parts[:2] + [hi, lo, hi, pad], 0)

    return rows


def sweep(start, terms, finish):
    carry = {}
    first = {}
    for i in range(start, start + HALF, 2):
        outs = []
        for rows, lhs, _ in terms:
            rhs = jnp.concatenate([rows(i), rows(i + HALF)], 1)
            outs.append(jnp.dot(lhs, rhs, preferred_element_type=F32))
        for h in range(2):
            for t in range(2):
                r = i + t + h * HALF
                part = []
                for b in range(2):
                    g = []
                    for e in range(2):
                        j = 32 * t + 16 * b + 8 * e
                        block = [
                            scale[tile(r), :] * out[j : j + 8, h * COLS : (h + 1) * COLS]
                            for (_, _, scale), out in zip(terms, outs)
                        ]
                        g.append(sum(block[1:], block[0]))
                    part.append(g[0] + lane_down(g[1]))
                if i + t == start:
                    first[h] = part[0]
                else:
                    finish(r, part[0] + carry[h])
                carry[h] = part[1]
    finish(start, first[0] + carry[1])
    finish(start + HALF, first[1] + carry[0])


def weights_of(a_ref, n):
    return a_ref[64 * n : 64 * n + 64, :]


def inner_pass(a_ref, si, e, m, u, w, ei_out, h_out):
    def finish(r, force):
        at = tile(r)
        rest = e[at, :] - m[at, :] * force
        ei_out[at, :] = rest
        h_out[at, :] = u[at, :] + (w[at, :] + rest)

    sweep(2, [(tile_rows(lambda r: u[tile(r), :]), weights_of(a_ref, 0), si)], finish)


def send_edges(u, h, x_msg, d_msg):
    for base, src in ((0, u), (3, h)):
        for c in range(3):
            x_msg[base + c] = src[every(2 * c), :]
            d_msg[base + c] = src[every(2 * c + 1), :]


def blank_pads(*refs):
    zero = jnp.zeros((ROWS, COLS), F32)
    for q in (6, 7):
        for ref in refs:
            ref[every(q), :] = zero


def prep_body(
    count_ref, place_ref, kmat_h, row_h, col_h, u_h, scale_h, v_h, mass_h, ext_h,
    x_msg, d_msg, u_t, w_t, e_t, m_t, ei_t, h_t, si_t, a_out,
    kmat, row, col, u_n, scale, v_n, mass, ext_n, sems,
):
    pairs = [
        (kmat_h, kmat), (row_h, row), (col_h, col), (u_h, u_n),
        (scale_h, scale), (v_h, v_n), (mass_h, mass), (ext_h, ext_n),
    ]
    copies = [pltpu.make_async_copy(a, b, sems.at[n]) for n, (a, b) in enumerate(pairs)]
    for copy in copies:
        copy.start()
    blank_pads(u_t, w_t, e_t, m_t, si_t)
    odd = place_ref[0] % 2 == 1
    dt = step_size(count_ref)[0:1]
    high = lax.Precision.HIGHEST
    for copy in copies[:3]:
        copy.wait()
    slot = lax.broadcasted_iota(jnp.int32, (64, WIDTH), 1)
    low = ((slot >= 64) & (slot < 96)) | (slot >= 128)
    full = []
    for layer in range(2):
        flip = odd if layer == 0 else jnp.logical_not(odd)
        rows = jnp.dot(
            jnp.where(flip, row[1], row[0]), kmat[...], precision=high, preferred_element_type=F32
        )
        cols = [jnp.where(flip, col[1, t], col[0, t]) for t in range(2)]
        blocks = [jnp.dot(rows, c, precision=high, preferred_element_type=F32) for c in cols]
        block = jnp.concatenate(blocks, 0)
        big = block.astype(BF16).astype(F32)
        full.append(jnp.where(low, block - big, big).astype(BF16))
    across = (lax.broadcasted_iota(jnp.int32, (64, WIDTH), 0) % 2) == 0
    a_out[0:64, :] = full[0]
    a_out[64:128, :] = full[1]
    a_out[128:192, :] = jnp.where(across, full[1].astype(F32), 0.0).astype(BF16)
    a_out[192:256, :] = jnp.where(across, 0.0, full[1].astype(F32)).astype(BF16)

    def sides(ref, k=None):
        low_plane, top_plane = (ref[0], ref[1]) if k is None else (ref[2 * k], ref[2 * k + 1])
        return jnp.where(odd, top_plane, low_plane), jnp.where(odd, low_plane, top_plane)

    for copy in copies[3:]:
        copy.wait()
    inv = [(dt * dt) / part for part in sides(mass)]
    for c in range(3):
        us, vs, es = sides(u_n, c), sides(v_n, c), sides(ext_n, c)
        for x in range(2):
            at = every(2 * c + x)
            u_t[at, :] = us[x]
            w_t[at, :] = dt * vs[x]
            e_t[at, :] = inv[x] * es[x]
            m_t[at, :] = inv[x]
            si_t[at, :] = scale[0]
    inner_pass(a_out, si_t, e_t, m_t, u_t, w_t, ei_t, h_t)
    send_edges(u_t, h_t, x_msg, d_msg)
    x_msg[6] = inv[0]
    d_msg[6] = inv[1]
    x_msg[7] = scale[1]
    d_msg[7] = scale[1]


def taken(rnd, x):
    sub = lax.broadcasted_iota(jnp.int32, (8, COLS), 0)
    return (sub % 2 == x) & (sub < 6)


def outer_step(rnd, x, planes, scale, count_ref, refs):
    u_t, w_t, m_t, ei_t, h_t, a_ref, s_t, mm_t, ur, hr, u1, w1 = refs
    act = jnp.where(count_ref[0] > 2 * rnd, 1.0, 0.0).astype(F32)
    mask = taken(rnd, 1 - x)
    for c in range(3):
        at = every(2 * c + 1 - x)
        ur[at, :] = planes(c)
        hr[at, :] = planes(3 + c)
        if rnd == 0:
            mm_t[at, :] = planes(6)
    if rnd == 0:
        blank_pads(s_t)
        for q in range(6):
            s_t[every(q), :] = scale
        for r in range(ROWS):
            mm_t[tile(r), :] = jnp.where(mask, mm_t[tile(r), :], m_t[tile(r), :])

    def get(r):
        return jnp.where(mask, ur[tile(r), :], u_t[tile(r), :])

    def finish(r, force):
        at = tile(r)
        pull = mm_t[at, :] * force
        u = get(r)
        goal = jnp.where(mask, hr[at, :], h_t[at, :])
        u1[at, :] = u + act * ((goal - pull) - u)
        w1[at, :] = w_t[at, :] + act * (ei_t[at, :] - pull)

    sweep(0, [(tile_rows(get), weights_of(a_ref, 1), s_t)], finish)


def within_body(rnd, *refs):
    refs = list(refs)
    take = lambda n: [refs.pop(0) for _ in range(n)]
    count_ref, place_ref, d_in, u_t, w_t, m_t, ei_t, h_t, a_ref = take(9)
    (scale,) = take(1) if rnd == 0 else (None,)
    if rnd > 0:
        sd_t, md_t = take(2)
    u1, w1, fd = take(3)
    if rnd == 0:
        sd_t, md_t = take(2)
    ur, hr = take(2)
    odd = place_ref[0] % 2 == 1
    layer = jnp.where(odd, d_in[7], scale[1]) if rnd == 0 else None
    outer_step(
        rnd, 1, lambda k: d_in[k], layer, count_ref,
        (u_t, w_t, m_t, ei_t, h_t, a_ref, sd_t, md_t, ur, hr, u1, w1),
    )

    def finish(r, force):
        fd[tile(r), :] = force

    sweep(1, [(tile_rows(lambda r: u1[tile(r), :]), weights_of(a_ref, 3), sd_t)], finish)


def across_body(rnd, *refs):
    refs = list(refs)
    take = lambda n: [refs.pop(0) for _ in range(n)]
    last = rnd == ROUNDS - 1
    count_ref, place_ref, x_in, u_t, w_t, e_t, m_t, ei_t, h_t, si_t, a_ref, u1d, w1d, fd = take(14)
    (scale,) = take(1) if rnd == 0 else (None,)
    if rnd > 0:
        sx_t, mx_t = take(2)
    if last:
        pick, share = take(2)
        u_out, v_out, g_out = take(3)
    else:
        x_msg, d_msg, u2, w2, ei_out, h_out = take(6)
    if rnd == 0:
        sx_t, mx_t = take(2)
    ur, hr, u1x, w1x, u1 = take(5)
    if last:
        u2, w2, u_nat, sem = take(4)
    place = place_ref[0]
    odd = place % 2 == 1
    inside = (place > 0) & (place < DOMS - 1)

    def planes(k):
        return jnp.where(inside, x_in[k], 0.0)

    layer = jnp.where(odd, scale[1], planes(7)) if rnd == 0 else None
    outer_step(
        rnd, 0, planes, layer, count_ref,
        (u_t, w_t, m_t, ei_t, h_t, a_ref, sx_t, mx_t, ur, hr, u1x, w1x),
    )
    act = jnp.where(count_ref[0] > 2 * rnd + 1, 1.0, 0.0).astype(F32)
    within = lax.broadcasted_iota(jnp.int32, (8, COLS), 0) % 2 == 1

    def middle(r):
        return jnp.where(within, u1d[tile(r), :], u1x[tile(r), :])

    def finish(r, force):
        at = tile(r)
        w = jnp.where(within, w1d[at, :], w1x[at, :])
        w = w + act * (e_t[at, :] - m_t[at, :] * (force + fd[at, :]))
        w2[at, :] = w
        u2[at, :] = middle(r) + act * w

    sweep(
        1,
        [
            (tile_rows(middle), weights_of(a_ref, 0), si_t),
            (tile_rows(lambda r: u1x[tile(r), :]), weights_of(a_ref, 2), sx_t),
        ],
        finish,
    )
    if last:
        back = step_size(count_ref)[0:1]
        for c in range(3):
            for src, out, scaled in ((u2, u_nat, False), (w2, v_out, True)):
                here, there = src[every(2 * c), :], src[every(2 * c + 1), :]
                if scaled:
                    here, there = here / back, there / back
                out[2 * c] = jnp.where(odd, there, here)
                out[2 * c + 1] = jnp.where(odd, here, there)
        copy = pltpu.make_async_copy(u_nat, u_out, sem)
        copy.start()
        partial_gaps(place_ref, pick, share, v_out, g_out)
        copy.wait()
        return
    inner_pass(a_ref, si_t, e_t, m_t, u2, w2, ei_out, h_out)
    send_edges(u2, h_out, x_msg, d_msg)


def thirds(x):
    parts = []
    for _ in range(3):
        part = x.astype(jnp.bfloat16)
        parts.append(part)
        x = x - part.astype(F32)
    return parts


def chosen(onehot, values):
    return sum(jnp.dot(onehot, part, preferred_element_type=F32) for part in thirds(values))


def node_body(own, peer, normal, before, mass, pick, pick_t, share, change):
    sub = lax.broadcasted_iota(jnp.int32, (16, 16), 0)
    eye = sub == lax.broadcasted_iota(jnp.int32, (16, 16), 1)
    lane = lax.broadcasted_iota(jnp.int32, (16, COLS), 1)
    weights = jnp.concatenate([mass[0], mass[1]], 1)

    def column(line):
        return jnp.sum(jnp.where(eye, jnp.broadcast_to(line, (16, 16)), 0.0), axis=1, keepdims=True)

    for side, nodes, vec, sign in ((0, own, normal, 1.0), (1, peer, before, -1.0)):
        at = slice(16 * side, 16 * side + 16)
        index = column(nodes[...].astype(F32)).astype(jnp.int32)
        plane = jnp.where(index >= ROWS * COLS, 1, 0)
        rest = index - plane * (ROWS * COLS)
        row = rest // COLS
        col = rest - row * COLS
        onehot = jnp.where(lane == row, 1.0, 0.0)
        pick[at, :] = onehot[:, 0:ROWS].astype(jnp.bfloat16)
        heavy = chosen(onehot[:, 0:ROWS].astype(jnp.bfloat16), weights)
        hits = [(lane == col) & (plane == p) for p in range(2)]
        total = jnp.where(hits[0], heavy[:, 0:COLS], 0.0) + jnp.where(hits[1], heavy[:, COLS:], 0.0)
        total = jnp.sum(total, axis=1, keepdims=True)
        for c in range(3):
            value = sign * column(vec[c : c + 1, :])
            for p in range(2):
                q = 2 * c + p
                part = jnp.where(hits[p], value, 0.0)
                share[at, q * COLS : (q + 1) * COLS] = part
                change[at, q * COLS : (q + 1) * COLS] = -part / total
        pick_t[side] = jnp.transpose(onehot)[0:ROWS].astype(jnp.bfloat16)


def partial_gaps(place_ref, pick, share, v, g_out):
    values = jnp.concatenate([v[q] for q in range(6)], 1)
    total = jnp.sum(chosen(pick[...], values) * share[...], axis=1, keepdims=True)
    lane = lax.broadcasted_iota(jnp.int32, (32, COLS), 1)
    sub = lax.broadcasted_iota(jnp.int32, (32, COLS), 0)
    line = jnp.where(lane == sub % 16 + 16 * (place_ref[0] % 8), jnp.broadcast_to(total, (32, COLS)), 0.0)
    for side in range(2):
        part = jnp.sum(line[16 * side : 16 * side + 16], axis=0, keepdims=True)
        g_out[:, side * COLS : (side + 1) * COLS] = jnp.broadcast_to(part, (128, COLS))


def final_body(gathered, inv_own, inv_before, pick_t, change, v_in, v_out):
    mine = jnp.sum(gathered[:, 0:COLS].reshape(16, 8, COLS), axis=1)
    other = jnp.sum(gathered[:, COLS : 2 * COLS].reshape(16, 8, COLS), axis=1)
    gap = mine + jnp.concatenate([other[4:16], other[0:4]], 0)
    total = None
    for side, rows in ((0, inv_own), (1, inv_before)):
        acc = jnp.zeros((16, COLS), F32)
        for k in range(16):
            acc = acc + rows[:, k * COLS : (k + 1) * COLS] * gap[k : k + 1, :]
        lam = jnp.sum(acc, axis=1, keepdims=True)
        part = chosen(pick_t[side], change[16 * side : 16 * side + 16, :] * lam)
        total = part if total is None else total + part
    for q in range(6):
        v_out[q] = v_in[q] + total[:, q * COLS : (q + 1) * COLS]


def call(body, outs, scratch, ins, limit=24 * 1024 * 1024, far_outs=()):
    return pl.pallas_call(
        body,
        out_shape=[s if isinstance(s, jax.ShapeDtypeStruct) else jax.ShapeDtypeStruct(s, F32) for s in outs],
        in_specs=ins,
        out_specs=[HBM if n in far_outs else VM for n in range(len(outs))],
        scratch_shapes=[pltpu.VMEM(s, F32) if isinstance(s, tuple) else s for s in scratch],
        compiler_params=pltpu.CompilerParams(vmem_limit_bytes=limit),
    )


TILE = (ROWS * 8, COLS)
PLANES = (6, ROWS, COLS)


def across_pairs():
    pairs = [(g * DOMS + i, g * DOMS + i + 1) for g in range(GROUPS) for i in range(1, DOMS - 1, 2)]
    for g in range(0, GROUPS, 2):
        for i in (0, DOMS - 1):
            pairs.append((g * DOMS + i, (g + 1) * DOMS + i))
    return pairs + [(b, a) for a, b in pairs]


ACROSS = across_pairs()
WITHIN = [(i, i ^ 1) for i in range(DOMS)]
FROM_BEFORE = [(i, (i + 1) % GROUPS) for i in range(GROUPS)]


def far(x):
    return pltpu.with_memory_space_constraint(jnp.asarray(x), pltpu.HBM)


def on_device(
    displacement, velocity, external, mass, elem_scale, stiffness, substeps,
    own_nodes, peer_nodes, normals, schur_inverse,
):
    field = displacement[0].reshape(PLANES)
    speed = velocity[0].reshape(PLANES)
    loads = external[0].reshape(PLANES)
    weight = mass[0]
    scale = elem_scale[0]
    place = lax.axis_index("dom").reshape(1)
    normal = normals[0]
    scalars = (substeps, place)
    b16 = lambda *shape: jax.ShapeDtypeStruct(shape, BF16)

    first = (8, ROWS, COLS)
    pair = (2, ROWS, COLS)
    x, d, u, w, e, m, ei, h, si, a = call(
        prep_body,
        [first, first] + [TILE] * 7 + [b16(256, WIDTH)],
        [
            (24, 24), (2, 32, 24), (2, 2, 24, WIDTH), PLANES, pair, PLANES, pair, PLANES,
            pltpu.SemaphoreType.DMA((8,)),
        ],
        [SM] * 2 + [HBM] * 8,
    )(*scalars, *(far(v) for v in (stiffness[0], PICK_ROW, PICK_COL, field, scale, speed, weight, loads)))
    for rnd in range(ROUNDS):
        last = rnd == ROUNDS - 1
        x = lax.ppermute(x, ("grp", "dom"), ACROSS)
        d = lax.ppermute(d, "dom", WITHIN)
        if rnd == 0:
            inv_before = lax.ppermute(schur_inverse, "grp", FROM_BEFORE)
            before = lax.ppermute(normal, "grp", FROM_BEFORE)

        def within(*refs, rnd=rnd):
            return within_body(rnd, *refs)

        args = [d, u, w, m, ei, h, a] + ([scale] if rnd == 0 else [sd, md])
        got = call(
            within, [TILE] * (5 if rnd == 0 else 3), [TILE] * 2, [SM] * 2 + [VM] * len(args)
        )(*scalars, *args)
        u1d, w1d, fd = got[:3]
        if rnd == 0:
            sd, md = got[3:]
            x, inv_before, before = lax.optimization_barrier((x, inv_before, before))
        if rnd == 1:
            nodes = call(
                node_body, [b16(32, ROWS), b16(2, ROWS, 16), (32, 6 * COLS), (32, 6 * COLS)], [], [VM] * 5
            )(own_nodes, peer_nodes, normal, before, weight)
            x, *nodes = lax.optimization_barrier((x, *nodes))
            pick, pick_t, share, change = nodes

        def across(*refs, rnd=rnd):
            return across_body(rnd, *refs)

        args = [x, u, w, e, m, ei, h, si, a, u1d, w1d, fd] + ([scale] if rnd == 0 else [sx, mx])
        args += [pick, share] if last else []
        outs = [PLANES, PLANES, (128, 2 * COLS)] if last else [PLANES, PLANES] + [TILE] * 4
        outs += [TILE, TILE] if rnd == 0 else []
        scratch = [TILE] * 5 + ([TILE, TILE, PLANES, pltpu.SemaphoreType.DMA] if last else [])
        got = call(
            across, outs, scratch, [SM] * 2 + [VM] * len(args), far_outs=(0,) if last else ()
        )(*scalars, *args)
        if last:
            u, v, gap = got
        else:
            x, d, u, w, ei, h = got[:6]
        if rnd == 0:
            sx, mx = got[6:]
    gathered = lax.all_to_all(gap, ("grp", "dom"), 0, 0, tiled=True)
    (v,) = call(final_body, [PLANES], [], [VM] * 6)(
        gathered, schur_inverse, inv_before, pick_t, change, v
    )
    shape = displacement.shape
    return u.reshape(shape), v.reshape(shape)


def solution(mesh):
    return jax.shard_map(
        on_device,
        mesh=mesh,
        in_specs=(
            P("grp", None, "dom", None, None),
            P("grp", None, "dom", None, None),
            P("grp", None, "dom", None, None),
            P("grp", "dom", None, None),
            P("grp", "dom", None, None),
            P("grp", None, None),
            P("grp"),
            P("grp", "dom"),
            P("grp", "dom"),
            P("grp", None, "dom"),
            P(("grp", "dom"), None),
        ),
        out_specs=(P("grp", None, "dom", None, None), P("grp", None, "dom", None, None)),
        check_vma=False,
    )
```

```python
import jax
import jax.numpy as jnp
import numpy as np
from jax import lax
from jax.experimental import pallas as pl
from jax.experimental.pallas import tpu as pltpu
from jax.sharding import PartitionSpec as P

MAXSUB = 8
ROUNDS = MAXSUB // 2
GROUPS = 4
DOMS = 32
COARSE = 0.4
ROWS = 96
HALF = ROWS // 2
COLS = 128
WIDTH = 256
F32 = jnp.float32
BF16 = jnp.bfloat16
VM = pl.BlockSpec(memory_space=pltpu.VMEM)
SM = pl.BlockSpec(memory_space=pltpu.SMEM)
HBM = pl.BlockSpec(memory_space=pltpu.HBM)


def describe():
    return [
        (at, q // 8, q % 8, part == 2) for at in range(3) for part in range(3) for q in range(16)
    ]


def selectors():
    pick_row = np.zeros((2, 32, 24), np.float32)
    pick_col = np.zeros((2, 2, 24, WIDTH), np.float32)
    for w in range(2):
        for be in range(4):
            for q in range(6):
                pick_row[w, be * 8 + q, (4 * (q % 2 ^ w) + be) * 3 + q // 2] = 1.0
        for t in range(2):
            for k, (at, e, q, _) in enumerate(describe()):
                if q < 6 and at - t in (0, 1):
                    pick_col[w, t, (4 * (q % 2 ^ w) + 2 * (at - t) + e) * 3 + q // 2, k] = 1.0
    return pick_row, pick_col


PICK_ROW, PICK_COL = selectors()


def step_size(count_ref):
    count = jnp.full((8, COLS), count_ref[0], jnp.int32).astype(F32)
    return COARSE / count


def lane_up(x):
    return pltpu.roll(x, COLS - 1, 1)


def lane_down(x):
    return pltpu.roll(x, 1, 1)


def every(i, stride=8):
    return pl.ds(i, ROWS, stride=stride)


def tile(r):
    return slice(8 * (r % ROWS), 8 * (r % ROWS) + 8)


def halves(u):
    hi = u.astype(BF16)
    return hi, (u - hi.astype(F32)).astype(BF16)


def tile_rows(get, rotated=None):
    done = {}

    def one(r):
        r %= ROWS
        if r not in done:
            here = get(r)
            shifted = lane_up(here) if rotated is None else rotated(r)
            done[r] = halves(jnp.concatenate([here, shifted], 0))
        hi, lo = done[r]
        return [hi, lo, hi]

    def rows(r):
        pad = jnp.zeros((WIDTH - 144, COLS), BF16)
        return jnp.concatenate(one(r) + one(r + 1) + one(r + 2) + [pad], 0)

    return rows


def sweep(start, terms, finish):
    carry = {}
    first = {}

    def close(r, a, b):
        finish(r, (a[0] + b[0]) + lane_down(a[1] + b[1]))

    for i in range(start, start + HALF, 2):
        outs = []
        for rows, lhs, _ in terms:
            rhs = jnp.concatenate([rows(i), rows(i + HALF)], 1)
            outs.append(jnp.dot(lhs, rhs, preferred_element_type=F32))
        for h in range(2):
            for t in range(2):
                r = i + t + h * HALF
                part = []
                for be in range(4):
                    j = 32 * t + 8 * be
                    block = [
                        scale[tile(r), :] * out[j : j + 8, h * COLS : (h + 1) * COLS]
                        for (_, _, scale), out in zip(terms, outs)
                    ]
                    part.append(sum(block[1:], block[0]))
                if i + t == start:
                    first[h] = part[:2]
                else:
                    close(r, part[:2], carry[h])
                carry[h] = part[2:]
    close(start, first[0], carry[1])
    close(start + HALF, first[1], carry[0])


def weights_of(a_ref, n):
    return a_ref[64 * n : 64 * n + 64, :]


def inner_pass(a_ref, si, e, m, u, w, ei_out, h_out):
    def finish(r, force):
        at = tile(r)
        rest = e[at, :] - m[at, :] * force
        ei_out[at, :] = rest
        h_out[at, :] = u[at, :] + (w[at, :] + rest)

    sweep(2, [(tile_rows(lambda r: u[tile(r), :]), weights_of(a_ref, 0), si)], finish)


def send_edges(u, h, x_msg, d_msg):
    for base, src in ((0, u), (3, h)):
        for c in range(3):
            x_msg[base + c] = src[every(2 * c), :]
            d_msg[base + c] = src[every(2 * c + 1), :]


def blank_pads(*refs):
    zero = jnp.zeros((ROWS, COLS), F32)
    for q in (6, 7):
        for ref in refs:
            ref[every(q), :] = zero


def prep_body(
    count_ref, place_ref, kmat_h, row_h, col_h, u_h, scale_h, v_h, mass_h, ext_h,
    x_msg, d_msg, u_t, w_t, e_t, m_t, ei_t, h_t, si_t, a_out,
    kmat, row, col, u_n, scale, v_n, mass, ext_n, sems,
):
    pairs = [
        (kmat_h, kmat), (row_h, row), (col_h, col), (u_h, u_n),
        (scale_h, scale), (v_h, v_n), (mass_h, mass), (ext_h, ext_n),
    ]
    copies = [pltpu.make_async_copy(a, b, sems.at[n]) for n, (a, b) in enumerate(pairs)]
    for copy in copies:
        copy.start()
    blank_pads(u_t, w_t, e_t, m_t, si_t)
    odd = place_ref[0] % 2 == 1
    dt = step_size(count_ref)[0:1]
    high = lax.Precision.HIGHEST
    for copy in copies[:3]:
        copy.wait()
    slot = lax.broadcasted_iota(jnp.int32, (64, WIDTH), 1)
    low = slot % 48 >= 32
    full = []
    for layer in range(2):
        flip = odd if layer == 0 else jnp.logical_not(odd)
        rows = jnp.dot(
            jnp.where(flip, row[1], row[0]), kmat[...], precision=high, preferred_element_type=F32
        )
        cols = [jnp.where(flip, col[1, t], col[0, t]) for t in range(2)]
        blocks = [jnp.dot(rows, c, precision=high, preferred_element_type=F32) for c in cols]
        block = jnp.concatenate(blocks, 0)
        big = block.astype(BF16).astype(F32)
        full.append(jnp.where(low, block - big, big).astype(BF16))
    across = (lax.broadcasted_iota(jnp.int32, (64, WIDTH), 0) % 2) == 0
    a_out[0:64, :] = full[0]
    a_out[64:128, :] = full[1]
    a_out[128:192, :] = jnp.where(across, full[1].astype(F32), 0.0).astype(BF16)
    a_out[192:256, :] = jnp.where(across, 0.0, full[1].astype(F32)).astype(BF16)

    def sides(ref, k=None):
        low_plane, top_plane = (ref[0], ref[1]) if k is None else (ref[2 * k], ref[2 * k + 1])
        return jnp.where(odd, top_plane, low_plane), jnp.where(odd, low_plane, top_plane)

    for copy in copies[3:]:
        copy.wait()
    inv = [(dt * dt) / part for part in sides(mass)]
    for c in range(3):
        us, vs, es = sides(u_n, c), sides(v_n, c), sides(ext_n, c)
        for x in range(2):
            at = every(2 * c + x)
            u_t[at, :] = us[x]
            w_t[at, :] = dt * vs[x]
            e_t[at, :] = inv[x] * es[x]
            m_t[at, :] = inv[x]
            si_t[at, :] = scale[0]
    inner_pass(a_out, si_t, e_t, m_t, u_t, w_t, ei_t, h_t)
    send_edges(u_t, h_t, x_msg, d_msg)
    x_msg[6] = inv[0]
    d_msg[6] = inv[1]
    x_msg[7] = scale[1]
    d_msg[7] = scale[1]


def taken(rnd, x):
    sub = lax.broadcasted_iota(jnp.int32, (8, COLS), 0)
    return (sub % 2 == x) & (sub < 6)


def outer_step(rnd, x, planes, scale, count_ref, refs):
    u_t, w_t, m_t, ei_t, h_t, a_ref, s_t, mm_t, ur, hr, u1, w1 = refs
    act = jnp.where(count_ref[0] > 2 * rnd, 1.0, 0.0).astype(F32)
    mask = taken(rnd, 1 - x)
    for c in range(3):
        at = every(2 * c + 1 - x)
        ur[at, :] = planes(c)
        hr[at, :] = planes(3 + c)
        if rnd == 0:
            mm_t[at, :] = planes(6)
    if rnd == 0:
        blank_pads(s_t)
        for q in range(6):
            s_t[every(q), :] = scale
        for r in range(ROWS):
            mm_t[tile(r), :] = jnp.where(mask, mm_t[tile(r), :], m_t[tile(r), :])

    def get(r):
        return jnp.where(mask, ur[tile(r), :], u_t[tile(r), :])

    def finish(r, force):
        at = tile(r)
        pull = mm_t[at, :] * force
        u = get(r)
        goal = jnp.where(mask, hr[at, :], h_t[at, :])
        u1[at, :] = u + act * ((goal - pull) - u)
        w1[at, :] = w_t[at, :] + act * (ei_t[at, :] - pull)

    sweep(0, [(tile_rows(get), weights_of(a_ref, 1), s_t)], finish)


def within_body(rnd, *refs):
    refs = list(refs)
    take = lambda n: [refs.pop(0) for _ in range(n)]
    count_ref, place_ref, d_in, u_t, w_t, m_t, ei_t, h_t, a_ref = take(9)
    (scale,) = take(1) if rnd == 0 else (None,)
    if rnd > 0:
        sd_t, md_t = take(2)
    u1, w1, fd, u1_shift = take(4)
    if rnd == 0:
        sd_t, md_t = take(2)
    ur, hr = take(2)
    odd = place_ref[0] % 2 == 1
    layer = jnp.where(odd, d_in[7], scale[1]) if rnd == 0 else None
    outer_step(
        rnd, 1, lambda k: d_in[k], layer, count_ref,
        (u_t, w_t, m_t, ei_t, h_t, a_ref, sd_t, md_t, ur, hr, u1, w1),
    )

    def finish(r, force):
        fd[tile(r), :] = force

    def rotated(r):
        u1_shift[tile(r), :] = lane_up(u1[tile(r), :])
        return u1_shift[tile(r), :]

    rows = tile_rows(lambda r: u1[tile(r), :], rotated)
    sweep(1, [(rows, weights_of(a_ref, 3), sd_t)], finish)


def across_body(rnd, *refs):
    refs = list(refs)
    take = lambda n: [refs.pop(0) for _ in range(n)]
    last = rnd == ROUNDS - 1
    count_ref, place_ref, x_in, u_t, w_t, e_t, m_t, ei_t, h_t, si_t, a_ref, u1d, w1d, fd, u1d_shift = take(15)
    (scale,) = take(1) if rnd == 0 else (None,)
    if rnd > 0:
        sx_t, mx_t = take(2)
    if last:
        pick, share = take(2)
        u_out, v_out, g_out = take(3)
    else:
        x_msg, d_msg, u2, w2, ei_out, h_out = take(6)
    if rnd == 0:
        sx_t, mx_t = take(2)
    ur, hr, u1x, w1x, u1 = take(5)
    if last:
        u2, w2, u_nat, sem = take(4)
    place = place_ref[0]
    odd = place % 2 == 1
    inside = (place > 0) & (place < DOMS - 1)

    def planes(k):
        return jnp.where(inside, x_in[k], 0.0)

    layer = jnp.where(odd, scale[1], planes(7)) if rnd == 0 else None
    outer_step(
        rnd, 0, planes, layer, count_ref,
        (u_t, w_t, m_t, ei_t, h_t, a_ref, sx_t, mx_t, ur, hr, u1x, w1x),
    )
    act = jnp.where(count_ref[0] > 2 * rnd + 1, 1.0, 0.0).astype(F32)
    within = lax.broadcasted_iota(jnp.int32, (8, COLS), 0) % 2 == 1

    def middle(r):
        return jnp.where(within, u1d[tile(r), :], u1x[tile(r), :])

    def finish(r, force):
        at = tile(r)
        w = jnp.where(within, w1d[at, :], w1x[at, :])
        w = w + act * (e_t[at, :] - m_t[at, :] * (force + fd[at, :]))
        w2[at, :] = w
        u2[at, :] = middle(r) + act * w

    shifts = {}

    def shift_x(r):
        if r not in shifts:
            shifts[r] = lane_up(u1x[tile(r), :])
        return shifts[r]

    def shift_middle(r):
        return jnp.where(within, u1d_shift[tile(r), :], shift_x(r))

    sweep(
        1,
        [
            (tile_rows(middle, shift_middle), weights_of(a_ref, 0), si_t),
            (tile_rows(lambda r: u1x[tile(r), :], shift_x), weights_of(a_ref, 2), sx_t),
        ],
        finish,
    )
    if last:
        back = step_size(count_ref)[0:1]
        for c in range(3):
            for src, out, scaled in ((u2, u_nat, False), (w2, v_out, True)):
                here, there = src[every(2 * c), :], src[every(2 * c + 1), :]
                if scaled:
                    here, there = here / back, there / back
                out[2 * c] = jnp.where(odd, there, here)
                out[2 * c + 1] = jnp.where(odd, here, there)
        copy = pltpu.make_async_copy(u_nat, u_out, sem)
        copy.start()
        partial_gaps(place_ref, pick, share, v_out, g_out)
        copy.wait()
        return
    inner_pass(a_ref, si_t, e_t, m_t, u2, w2, ei_out, h_out)
    send_edges(u2, h_out, x_msg, d_msg)


def thirds(x):
    parts = []
    for _ in range(3):
        part = x.astype(jnp.bfloat16)
        parts.append(part)
        x = x - part.astype(F32)
    return parts


def chosen(onehot, values):
    return sum(jnp.dot(onehot, part, preferred_element_type=F32) for part in thirds(values))


def node_body(own, peer, normal, before, mass, pick, pick_t, share, change):
    sub = lax.broadcasted_iota(jnp.int32, (16, 16), 0)
    eye = sub == lax.broadcasted_iota(jnp.int32, (16, 16), 1)
    lane = lax.broadcasted_iota(jnp.int32, (16, COLS), 1)
    weights = jnp.concatenate([mass[0], mass[1]], 1)

    def column(line):
        return jnp.sum(jnp.where(eye, jnp.broadcast_to(line, (16, 16)), 0.0), axis=1, keepdims=True)

    for side, nodes, vec, sign in ((0, own, normal, 1.0), (1, peer, before, -1.0)):
        at = slice(16 * side, 16 * side + 16)
        index = column(nodes[...].astype(F32)).astype(jnp.int32)
        plane = jnp.where(index >= ROWS * COLS, 1, 0)
        rest = index - plane * (ROWS * COLS)
        row = rest // COLS
        col = rest - row * COLS
        onehot = jnp.where(lane == row, 1.0, 0.0)
        pick[at, :] = onehot[:, 0:ROWS].astype(jnp.bfloat16)
        heavy = chosen(onehot[:, 0:ROWS].astype(jnp.bfloat16), weights)
        hits = [(lane == col) & (plane == p) for p in range(2)]
        total = jnp.where(hits[0], heavy[:, 0:COLS], 0.0) + jnp.where(hits[1], heavy[:, COLS:], 0.0)
        total = jnp.sum(total, axis=1, keepdims=True)
        for c in range(3):
            value = sign * column(vec[c : c + 1, :])
            for p in range(2):
                q = 2 * c + p
                part = jnp.where(hits[p], value, 0.0)
                share[at, q * COLS : (q + 1) * COLS] = part
                change[at, q * COLS : (q + 1) * COLS] = -part / total
        pick_t[side] = jnp.transpose(onehot)[0:ROWS].astype(jnp.bfloat16)


def partial_gaps(place_ref, pick, share, v, g_out):
    values = jnp.concatenate([v[q] for q in range(6)], 1)
    total = jnp.sum(chosen(pick[...], values) * share[...], axis=1, keepdims=True)
    lane = lax.broadcasted_iota(jnp.int32, (32, COLS), 1)
    sub = lax.broadcasted_iota(jnp.int32, (32, COLS), 0)
    line = jnp.where(lane == sub % 16 + 16 * (place_ref[0] % 8), jnp.broadcast_to(total, (32, COLS)), 0.0)
    for side in range(2):
        part = jnp.sum(line[16 * side : 16 * side + 16], axis=0, keepdims=True)
        g_out[:, side * COLS : (side + 1) * COLS] = jnp.broadcast_to(part, (128, COLS))


def final_body(gathered, inv_own, inv_before, pick_t, change, v_in, v_out):
    mine = jnp.sum(gathered[:, 0:COLS].reshape(16, 8, COLS), axis=1)
    other = jnp.sum(gathered[:, COLS : 2 * COLS].reshape(16, 8, COLS), axis=1)
    gap = mine + jnp.concatenate([other[4:16], other[0:4]], 0)
    total = None
    for side, rows in ((0, inv_own), (1, inv_before)):
        acc = jnp.zeros((16, COLS), F32)
        for k in range(16):
            acc = acc + rows[:, k * COLS : (k + 1) * COLS] * gap[k : k + 1, :]
        lam = jnp.sum(acc, axis=1, keepdims=True)
        part = chosen(pick_t[side], change[16 * side : 16 * side + 16, :] * lam)
        total = part if total is None else total + part
    for q in range(6):
        v_out[q] = v_in[q] + total[:, q * COLS : (q + 1) * COLS]


def call(body, outs, scratch, ins, limit=24 * 1024 * 1024, far_outs=()):
    return pl.pallas_call(
        body,
        out_shape=[s if isinstance(s, jax.ShapeDtypeStruct) else jax.ShapeDtypeStruct(s, F32) for s in outs],
        in_specs=ins,
        out_specs=[HBM if n in far_outs else VM for n in range(len(outs))],
        scratch_shapes=[pltpu.VMEM(s, F32) if isinstance(s, tuple) else s for s in scratch],
        compiler_params=pltpu.CompilerParams(vmem_limit_bytes=limit),
    )


TILE = (ROWS * 8, COLS)
PLANES = (6, ROWS, COLS)


def across_pairs():
    pairs = [(g * DOMS + i, g * DOMS + i + 1) for g in range(GROUPS) for i in range(1, DOMS - 1, 2)]
    for g in range(0, GROUPS, 2):
        for i in (0, DOMS - 1):
            pairs.append((g * DOMS + i, (g + 1) * DOMS + i))
    return pairs + [(b, a) for a, b in pairs]


ACROSS = across_pairs()
WITHIN = [(i, i ^ 1) for i in range(DOMS)]
FROM_BEFORE = [(i, (i + 1) % GROUPS) for i in range(GROUPS)]


def far(x):
    return pltpu.with_memory_space_constraint(jnp.asarray(x), pltpu.HBM)


def on_device(
    displacement, velocity, external, mass, elem_scale, stiffness, substeps,
    own_nodes, peer_nodes, normals, schur_inverse,
):
    field = displacement[0].reshape(PLANES)
    speed = velocity[0].reshape(PLANES)
    loads = external[0].reshape(PLANES)
    weight = mass[0]
    scale = elem_scale[0]
    place = lax.axis_index("dom").reshape(1)
    normal = normals[0]
    scalars = (substeps, place)
    b16 = lambda *shape: jax.ShapeDtypeStruct(shape, BF16)

    first = (8, ROWS, COLS)
    pair = (2, ROWS, COLS)
    x, d, u, w, e, m, ei, h, si, a = call(
        prep_body,
        [first, first] + [TILE] * 7 + [b16(256, WIDTH)],
        [
            (24, 24), (2, 32, 24), (2, 2, 24, WIDTH), PLANES, pair, PLANES, pair, PLANES,
            pltpu.SemaphoreType.DMA((8,)),
        ],
        [SM] * 2 + [HBM] * 8,
    )(*scalars, *(far(v) for v in (stiffness[0], PICK_ROW, PICK_COL, field, scale, speed, weight, loads)))
    for rnd in range(ROUNDS):
        last = rnd == ROUNDS - 1
        x = lax.ppermute(x, ("grp", "dom"), ACROSS)
        d = lax.ppermute(d, "dom", WITHIN)
        if rnd == 0:
            inv_before = lax.ppermute(schur_inverse, "grp", FROM_BEFORE)
            before = lax.ppermute(normal, "grp", FROM_BEFORE)
            d, inv_before, before = lax.optimization_barrier((d, inv_before, before))

        if rnd == 1:
            nodes = call(
                node_body, [b16(32, ROWS), b16(2, ROWS, 16), (32, 6 * COLS), (32, 6 * COLS)], [], [VM] * 5
            )(own_nodes, peer_nodes, normal, before, weight)
            d, *nodes = lax.optimization_barrier((d, *nodes))
            pick, pick_t, share, change = nodes

        def within(*refs, rnd=rnd):
            return within_body(rnd, *refs)

        args = [d, u, w, m, ei, h, a] + ([scale] if rnd == 0 else [sd, md])
        got = call(
            within, [TILE] * (6 if rnd == 0 else 4), [TILE] * 2, [SM] * 2 + [VM] * len(args)
        )(*scalars, *args)
        u1d, w1d, fd, u1d_shift = got[:4]
        if rnd == 0:
            sd, md = got[4:]

        def across(*refs, rnd=rnd):
            return across_body(rnd, *refs)

        args = [x, u, w, e, m, ei, h, si, a, u1d, w1d, fd, u1d_shift] + ([scale] if rnd == 0 else [sx, mx])
        args += [pick, share] if last else []
        outs = [PLANES, PLANES, (128, 2 * COLS)] if last else [PLANES, PLANES] + [TILE] * 4
        outs += [TILE, TILE] if rnd == 0 else []
        scratch = [TILE] * 5 + ([TILE, TILE, PLANES, pltpu.SemaphoreType.DMA] if last else [])
        got = call(
            across, outs, scratch, [SM] * 2 + [VM] * len(args), far_outs=(0,) if last else ()
        )(*scalars, *args)
        if last:
            u, v, gap = got
        else:
            x, d, u, w, ei, h = got[:6]
        if rnd == 0:
            sx, mx = got[6:]
    gathered = lax.all_to_all(gap, ("grp", "dom"), 0, 0, tiled=True)
    (v,) = call(final_body, [PLANES], [], [VM] * 6)(
        gathered, schur_inverse, inv_before, pick_t, change, v
    )
    shape = displacement.shape
    return u.reshape(shape), v.reshape(shape)


def solution(mesh):
    return jax.shard_map(
        on_device,
        mesh=mesh,
        in_specs=(
            P("grp", None, "dom", None, None),
            P("grp", None, "dom", None, None),
            P("grp", None, "dom", None, None),
            P("grp", "dom", None, None),
            P("grp", "dom", None, None),
            P("grp", None, None),
            P("grp"),
            P("grp", "dom"),
            P("grp", "dom"),
            P("grp", None, "dom"),
            P(("grp", "dom"), None),
        ),
        out_specs=(P("grp", None, "dom", None, None), P("grp", None, "dom", None, None)),
        check_vma=False,
    )
```

```python
import jax
import jax.numpy as jnp
import numpy as np
from jax import lax
from jax.experimental import pallas as pl
from jax.experimental.pallas import tpu as pltpu
from jax.sharding import PartitionSpec as P


MAXSUB = 8
ROUNDS = MAXSUB // 2
GROUPS = 4
DOMS = 32
COARSE = 0.4
ROWS = 96
HALF = ROWS // 2
COLS = 128
WIDTH = 256
F32 = jnp.float32
BF16 = jnp.bfloat16
VM = pl.BlockSpec(memory_space=pltpu.VMEM)
SM = pl.BlockSpec(memory_space=pltpu.SMEM)
HBM = pl.BlockSpec(memory_space=pltpu.HBM)


def describe():
    return [
        (at, q // 8, q % 8, part == 2) for at in range(3) for part in range(3) for q in range(16)
    ]


def selectors():
    pick_row = np.zeros((2, 32, 24), np.float32)
    pick_col = np.zeros((2, 2, 24, WIDTH), np.float32)
    for w in range(2):
        for be in range(4):
            for q in range(6):
                pick_row[w, be * 8 + q, (4 * (q % 2 ^ w) + be) * 3 + q // 2] = 1.0
        for t in range(2):
            for k, (at, e, q, _) in enumerate(describe()):
                if q < 6 and at - t in (0, 1):
                    pick_col[w, t, (4 * (q % 2 ^ w) + 2 * (at - t) + e) * 3 + q // 2, k] = 1.0
    return pick_row, pick_col


PICK_ROW, PICK_COL = selectors()


def step_size(count_ref):
    count = jnp.full((8, COLS), count_ref[0], jnp.int32).astype(F32)
    return COARSE / count


def lane_up(x):
    return pltpu.roll(x, COLS - 1, 1)


def lane_down(x):
    return pltpu.roll(x, 1, 1)


def every(i, stride=8):
    return pl.ds(i, ROWS, stride=stride)


def tile(r):
    return slice(8 * (r % ROWS), 8 * (r % ROWS) + 8)


def halves(u):
    hi = u.astype(BF16)
    return hi, (u - hi.astype(F32)).astype(BF16)


def tile_rows(get, rotated=None):
    done = {}

    def one(r):
        r %= ROWS
        if r not in done:
            here = get(r)
            shifted = lane_up(here) if rotated is None else rotated(r)
            done[r] = halves(jnp.concatenate([here, shifted], 0))
        hi, lo = done[r]
        return [hi, lo, hi]

    def rows(r):
        pad = jnp.zeros((WIDTH - 144, COLS), BF16)
        return jnp.concatenate(one(r) + one(r + 1) + one(r + 2) + [pad], 0)

    return rows


def sweep(start, terms, finish):
    carry = {}
    first = {}

    def close(r, a, b):
        finish(r, (a[0] + b[0]) + lane_down(a[1] + b[1]))

    for i in range(start, start + HALF, 2):
        outs = []
        for rows, lhs, _ in terms:
            rhs = jnp.concatenate([rows(i), rows(i + HALF)], 1)
            outs.append(jnp.dot(lhs, rhs, preferred_element_type=F32))
        for h in range(2):
            for t in range(2):
                r = i + t + h * HALF
                part = []
                for be in range(4):
                    j = 32 * t + 8 * be
                    block = [
                        scale[tile(r), :] * out[j : j + 8, h * COLS : (h + 1) * COLS]
                        for (_, _, scale), out in zip(terms, outs)
                    ]
                    part.append(sum(block[1:], block[0]))
                if i + t == start:
                    first[h] = part[:2]
                else:
                    close(r, part[:2], carry[h])
                carry[h] = part[2:]
    close(start, first[0], carry[1])
    close(start + HALF, first[1], carry[0])


def weights_of(a_ref, n):
    return a_ref[64 * n : 64 * n + 64, :]


def inner_pass(a_ref, si, e, m, u, w, ei_out, h_out):
    def finish(r, force):
        at = tile(r)
        rest = e[at, :] - m[at, :] * force
        ei_out[at, :] = rest
        h_out[at, :] = u[at, :] + (w[at, :] + rest)

    sweep(2, [(tile_rows(lambda r: u[tile(r), :]), weights_of(a_ref, 0), si)], finish)


def send_edges(u, h, x_msg, d_msg):
    for base, src in ((0, u), (3, h)):
        for c in range(3):
            x_msg[base + c] = src[every(2 * c), :]
            d_msg[base + c] = src[every(2 * c + 1), :]


def blank_pads(*refs):
    zero = jnp.zeros((ROWS, COLS), F32)
    for q in (6, 7):
        for ref in refs:
            ref[every(q), :] = zero


def prep_body(
    count_ref, place_ref, kmat_h, row_h, col_h, u_h, scale_h, v_h, mass_h, ext_h,
    x_msg, d_msg, u_t, w_t, e_t, m_t, ei_t, h_t, si_t, a_out,
    kmat, row, col, u_n, scale, v_n, mass, ext_n, sems,
):
    pairs = [
        (kmat_h, kmat), (row_h, row), (col_h, col), (u_h, u_n),
        (scale_h, scale), (v_h, v_n), (mass_h, mass), (ext_h, ext_n),
    ]
    copies = [pltpu.make_async_copy(a, b, sems.at[n]) for n, (a, b) in enumerate(pairs)]
    for copy in copies:
        copy.start()
    blank_pads(u_t, w_t, e_t, m_t, si_t)
    odd = place_ref[0] % 2 == 1
    dt = step_size(count_ref)[0:1]
    high = lax.Precision.HIGHEST
    for copy in copies[:3]:
        copy.wait()
    slot = lax.broadcasted_iota(jnp.int32, (64, WIDTH), 1)
    low = slot % 48 >= 32
    full = []
    for layer in range(2):
        flip = odd if layer == 0 else jnp.logical_not(odd)
        rows = jnp.dot(
            jnp.where(flip, row[1], row[0]), kmat[...], precision=high, preferred_element_type=F32
        )
        cols = [jnp.where(flip, col[1, t], col[0, t]) for t in range(2)]
        blocks = [jnp.dot(rows, c, precision=high, preferred_element_type=F32) for c in cols]
        block = jnp.concatenate(blocks, 0)
        big = block.astype(BF16).astype(F32)
        full.append(jnp.where(low, block - big, big).astype(BF16))
    across = (lax.broadcasted_iota(jnp.int32, (64, WIDTH), 0) % 2) == 0
    a_out[0:64, :] = full[0]
    a_out[64:128, :] = full[1]
    a_out[128:192, :] = jnp.where(across, full[1].astype(F32), 0.0).astype(BF16)
    a_out[192:256, :] = jnp.where(across, 0.0, full[1].astype(F32)).astype(BF16)

    def sides(ref, k=None):
        low_plane, top_plane = (ref[0], ref[1]) if k is None else (ref[2 * k], ref[2 * k + 1])
        return jnp.where(odd, top_plane, low_plane), jnp.where(odd, low_plane, top_plane)

    for copy in copies[3:]:
        copy.wait()
    inv = [(dt * dt) / part for part in sides(mass)]
    for c in range(3):
        us, vs, es = sides(u_n, c), sides(v_n, c), sides(ext_n, c)
        for x in range(2):
            at = every(2 * c + x)
            u_t[at, :] = us[x]
            w_t[at, :] = dt * vs[x]
            e_t[at, :] = inv[x] * es[x]
            m_t[at, :] = inv[x]
            si_t[at, :] = scale[0]
    inner_pass(a_out, si_t, e_t, m_t, u_t, w_t, ei_t, h_t)
    send_edges(u_t, h_t, x_msg, d_msg)
    x_msg[6] = inv[0]
    d_msg[6] = inv[1]
    x_msg[7] = scale[1]
    d_msg[7] = scale[1]


def taken(x):
    sub = lax.broadcasted_iota(jnp.int32, (8, COLS), 0)
    return (sub % 2 == x) & (sub < 6)


def outer_step(rnd, x, planes, scale, count_ref, refs):
    u_t, w_t, m_t, ei_t, h_t, a_ref, s_t, mm_t, ur, hr, u1, w1 = refs
    act = jnp.where(count_ref[0] > 2 * rnd, 1.0, 0.0).astype(F32)
    mask = taken(1 - x)
    for c in range(3):
        at = every(2 * c + 1 - x)
        ur[at, :] = planes(c)
        hr[at, :] = planes(3 + c)
        if rnd == 0:
            mm_t[at, :] = planes(6)
    if rnd == 0:
        blank_pads(s_t)
        for q in range(6):
            s_t[every(q), :] = scale
        for r in range(ROWS):
            mm_t[tile(r), :] = jnp.where(mask, mm_t[tile(r), :], m_t[tile(r), :])

    def get(r):
        return jnp.where(mask, ur[tile(r), :], u_t[tile(r), :])

    def finish(r, force):
        at = tile(r)
        pull = mm_t[at, :] * force
        u = get(r)
        goal = jnp.where(mask, hr[at, :], h_t[at, :])
        u1[at, :] = u + act * ((goal - pull) - u)
        w1[at, :] = w_t[at, :] + act * (ei_t[at, :] - pull)

    sweep(0, [(tile_rows(get), weights_of(a_ref, 1), s_t)], finish)


def within_body(rnd, *refs):
    refs = list(refs)
    take = lambda n: [refs.pop(0) for _ in range(n)]
    count_ref, place_ref, d_in, u_t, w_t, m_t, ei_t, h_t, a_ref = take(9)
    (scale,) = take(1) if rnd == 0 else (None,)
    if rnd > 0:
        sd_t, md_t = take(2)
    u1, w1, fd, u1_shift = take(4)
    if rnd == 0:
        sd_t, md_t = take(2)
    ur, hr = take(2)
    odd = place_ref[0] % 2 == 1
    layer = jnp.where(odd, d_in[7], scale[1]) if rnd == 0 else None
    outer_step(
        rnd, 1, lambda k: d_in[k], layer, count_ref,
        (u_t, w_t, m_t, ei_t, h_t, a_ref, sd_t, md_t, ur, hr, u1, w1),
    )

    def finish(r, force):
        fd[tile(r), :] = force

    def rotated(r):
        u1_shift[tile(r), :] = lane_up(u1[tile(r), :])
        return u1_shift[tile(r), :]

    rows = tile_rows(lambda r: u1[tile(r), :], rotated)
    sweep(1, [(rows, weights_of(a_ref, 3), sd_t)], finish)


def across_body(rnd, *refs):
    refs = list(refs)
    take = lambda n: [refs.pop(0) for _ in range(n)]
    last = rnd == ROUNDS - 1
    count_ref, place_ref, x_in, u_t, w_t, e_t, m_t, ei_t, h_t, si_t, a_ref, u1d, w1d, fd, u1d_shift = take(15)
    (scale,) = take(1) if rnd == 0 else (None,)
    if rnd > 0:
        sx_t, mx_t = take(2)
    if last:
        pick, share = take(2)
        u_out, v_out, g_out = take(3)
    else:
        x_msg, d_msg, u2, w2, ei_out, h_out = take(6)
    if rnd == 0:
        sx_t, mx_t = take(2)
    ur, hr, u1x, w1x, _ = take(5)
    if last:
        u2, w2, u_nat, sem = take(4)
    place = place_ref[0]
    odd = place % 2 == 1
    inside = (place > 0) & (place < DOMS - 1)

    def planes(k):
        return jnp.where(inside, x_in[k], 0.0)

    layer = jnp.where(odd, scale[1], planes(7)) if rnd == 0 else None
    outer_step(
        rnd, 0, planes, layer, count_ref,
        (u_t, w_t, m_t, ei_t, h_t, a_ref, sx_t, mx_t, ur, hr, u1x, w1x),
    )
    act = jnp.where(count_ref[0] > 2 * rnd + 1, 1.0, 0.0).astype(F32)
    within = lax.broadcasted_iota(jnp.int32, (8, COLS), 0) % 2 == 1

    def middle(r):
        return jnp.where(within, u1d[tile(r), :], u1x[tile(r), :])

    def finish(r, force):
        at = tile(r)
        w = jnp.where(within, w1d[at, :], w1x[at, :])
        w = w + act * (e_t[at, :] - m_t[at, :] * (force + fd[at, :]))
        w2[at, :] = w
        u2[at, :] = middle(r) + act * w

    shifts = {}

    def shift_x(r):
        if r not in shifts:
            shifts[r] = lane_up(u1x[tile(r), :])
        return shifts[r]

    def shift_middle(r):
        return jnp.where(within, u1d_shift[tile(r), :], shift_x(r))

    sweep(
        1,
        [
            (tile_rows(middle, shift_middle), weights_of(a_ref, 0), si_t),
            (tile_rows(lambda r: u1x[tile(r), :], shift_x), weights_of(a_ref, 2), sx_t),
        ],
        finish,
    )
    if last:
        back = step_size(count_ref)[0:1]
        for c in range(3):
            for src, out, scaled in ((u2, u_nat, False), (w2, v_out, True)):
                here, there = src[every(2 * c), :], src[every(2 * c + 1), :]
                if scaled:
                    here, there = here / back, there / back
                out[2 * c] = jnp.where(odd, there, here)
                out[2 * c + 1] = jnp.where(odd, here, there)
        copy = pltpu.make_async_copy(u_nat, u_out, sem)
        copy.start()
        partial_gaps(place_ref, pick, share, v_out, g_out)
        copy.wait()
        return
    inner_pass(a_ref, si_t, e_t, m_t, u2, w2, ei_out, h_out)
    send_edges(u2, h_out, x_msg, d_msg)


def thirds(x):
    parts = []
    for _ in range(3):
        part = x.astype(jnp.bfloat16)
        parts.append(part)
        x = x - part.astype(F32)
    return parts


def chosen(onehot, values):
    return sum(jnp.dot(onehot, part, preferred_element_type=F32) for part in thirds(values))


def node_body(own, peer, normal, before, mass, pick, pick_t, share, change):
    sub = lax.broadcasted_iota(jnp.int32, (16, 16), 0)
    eye = sub == lax.broadcasted_iota(jnp.int32, (16, 16), 1)
    lane = lax.broadcasted_iota(jnp.int32, (16, COLS), 1)
    weights = jnp.concatenate([mass[0], mass[1]], 1)

    def column(line):
        return jnp.sum(jnp.where(eye, jnp.broadcast_to(line, (16, 16)), 0.0), axis=1, keepdims=True)

    for side, nodes, vec, sign in ((0, own, normal, 1.0), (1, peer, before, -1.0)):
        at = slice(16 * side, 16 * side + 16)
        index = column(nodes[...].astype(F32)).astype(jnp.int32)
        plane = jnp.where(index >= ROWS * COLS, 1, 0)
        rest = index - plane * (ROWS * COLS)
        row = rest // COLS
        col = rest - row * COLS
        onehot = jnp.where(lane == row, 1.0, 0.0)
        pick[at, :] = onehot[:, 0:ROWS].astype(jnp.bfloat16)
        heavy = chosen(onehot[:, 0:ROWS].astype(jnp.bfloat16), weights)
        hits = [(lane == col) & (plane == p) for p in range(2)]
        total = jnp.where(hits[0], heavy[:, 0:COLS], 0.0) + jnp.where(hits[1], heavy[:, COLS:], 0.0)
        total = jnp.sum(total, axis=1, keepdims=True)
        for c in range(3):
            value = sign * column(vec[c : c + 1, :])
            for p in range(2):
                q = 2 * c + p
                part = jnp.where(hits[p], value, 0.0)
                share[at, q * COLS : (q + 1) * COLS] = part
                change[at, q * COLS : (q + 1) * COLS] = -part / total
        pick_t[side] = jnp.transpose(onehot)[0:ROWS].astype(jnp.bfloat16)


def partial_gaps(place_ref, pick, share, v, g_out):
    values = jnp.concatenate([v[q] for q in range(6)], 1)
    total = jnp.sum(chosen(pick[...], values) * share[...], axis=1, keepdims=True)
    lane = lax.broadcasted_iota(jnp.int32, (32, COLS), 1)
    sub = lax.broadcasted_iota(jnp.int32, (32, COLS), 0)
    line = jnp.where(lane == sub % 16 + 16 * (place_ref[0] % 8), jnp.broadcast_to(total, (32, COLS)), 0.0)
    for side in range(2):
        part = jnp.sum(line[16 * side : 16 * side + 16], axis=0, keepdims=True)
        g_out[:, side * COLS : (side + 1) * COLS] = jnp.broadcast_to(part, (128, COLS))


def final_body(gathered, inv_own, inv_before, pick_t, change, v_in, v_out):
    mine = jnp.sum(gathered[:, 0:COLS].reshape(16, 8, COLS), axis=1)
    other = jnp.sum(gathered[:, COLS : 2 * COLS].reshape(16, 8, COLS), axis=1)
    gap = mine + jnp.concatenate([other[4:16], other[0:4]], 0)
    total = None
    for side, rows in ((0, inv_own), (1, inv_before)):
        acc = jnp.zeros((16, COLS), F32)
        for k in range(16):
            acc = acc + rows[:, k * COLS : (k + 1) * COLS] * gap[k : k + 1, :]
        lam = jnp.sum(acc, axis=1, keepdims=True)
        part = chosen(pick_t[side], change[16 * side : 16 * side + 16, :] * lam)
        total = part if total is None else total + part
    for q in range(6):
        v_out[q] = v_in[q] + total[:, q * COLS : (q + 1) * COLS]


def call(body, outs, scratch, ins, limit=24 * 1024 * 1024, far_outs=()):
    return pl.pallas_call(
        body,
        out_shape=[s if isinstance(s, jax.ShapeDtypeStruct) else jax.ShapeDtypeStruct(s, F32) for s in outs],
        in_specs=ins,
        out_specs=[HBM if n in far_outs else VM for n in range(len(outs))],
        scratch_shapes=[pltpu.VMEM(s, F32) if isinstance(s, tuple) else s for s in scratch],
        compiler_params=pltpu.CompilerParams(vmem_limit_bytes=limit),
    )


TILE = (ROWS * 8, COLS)
PLANES = (6, ROWS, COLS)


def across_pairs():
    pairs = [(g * DOMS + i, g * DOMS + i + 1) for g in range(GROUPS) for i in range(1, DOMS - 1, 2)]
    for g in range(0, GROUPS, 2):
        for i in (0, DOMS - 1):
            pairs.append((g * DOMS + i, (g + 1) * DOMS + i))
    return pairs + [(b, a) for a, b in pairs]


ACROSS = across_pairs()
WITHIN = [(i, i ^ 1) for i in range(DOMS)]
FROM_BEFORE = [(i, (i + 1) % GROUPS) for i in range(GROUPS)]


def far(x):
    return pltpu.with_memory_space_constraint(jnp.asarray(x), pltpu.HBM)


def on_device(
    displacement, velocity, external, mass, elem_scale, stiffness, substeps,
    own_nodes, peer_nodes, normals, schur_inverse,
):
    field = displacement[0].reshape(PLANES)
    speed = velocity[0].reshape(PLANES)
    loads = external[0].reshape(PLANES)
    weight = mass[0]
    scale = elem_scale[0]
    place = lax.axis_index("dom").reshape(1)
    normal = normals[0]
    scalars = (substeps, place)
    b16 = lambda *shape: jax.ShapeDtypeStruct(shape, BF16)

    first = (8, ROWS, COLS)
    pair = (2, ROWS, COLS)
    x, d, u, w, e, m, ei, h, si, a = call(
        prep_body,
        [first, first] + [TILE] * 7 + [b16(256, WIDTH)],
        [
            (24, 24), (2, 32, 24), (2, 2, 24, WIDTH), PLANES, pair, PLANES, pair, PLANES,
            pltpu.SemaphoreType.DMA((8,)),
        ],
        [SM] * 2 + [HBM] * 8,
    )(*scalars, *(far(v) for v in (stiffness[0], PICK_ROW, PICK_COL, field, scale, speed, weight, loads)))
    for rnd in range(ROUNDS):
        last = rnd == ROUNDS - 1
        x = lax.ppermute(x, ("grp", "dom"), ACROSS)
        d = lax.ppermute(d, "dom", WITHIN)
        if rnd == 0:
            inv_before = lax.ppermute(schur_inverse, "grp", FROM_BEFORE)
            before = lax.ppermute(normal, "grp", FROM_BEFORE)

        if rnd == 1:
            nodes = call(
                node_body, [b16(32, ROWS), b16(2, ROWS, 16), (32, 6 * COLS), (32, 6 * COLS)], [], [VM] * 5
            )(own_nodes, peer_nodes, normal, before, weight)
            d, *nodes = lax.optimization_barrier((d, *nodes))
            pick, pick_t, share, change = nodes

        def within(*refs, rnd=rnd):
            return within_body(rnd, *refs)

        args = [d, u, w, m, ei, h, a] + ([scale] if rnd == 0 else [sd, md])
        got = call(
            within, [TILE] * (6 if rnd == 0 else 4), [TILE] * 2, [SM] * 2 + [VM] * len(args)
        )(*scalars, *args)
        u1d, w1d, fd, u1d_shift = got[:4]
        if rnd == 0:
            sd, md = got[4:]
            u1d, inv_before, before = lax.optimization_barrier((u1d, inv_before, before))

        def across(*refs, rnd=rnd):
            return across_body(rnd, *refs)

        args = [x, u, w, e, m, ei, h, si, a, u1d, w1d, fd, u1d_shift] + ([scale] if rnd == 0 else [sx, mx])
        args += [pick, share] if last else []
        outs = [PLANES, PLANES, (128, 2 * COLS)] if last else [PLANES, PLANES] + [TILE] * 4
        outs += [TILE, TILE] if rnd == 0 else []
        scratch = [TILE] * 5 + ([TILE, TILE, PLANES, pltpu.SemaphoreType.DMA] if last else [])
        got = call(
            across, outs, scratch, [SM] * 2 + [VM] * len(args), far_outs=(0,) if last else ()
        )(*scalars, *args)
        if last:
            u, v, gap = got
        else:
            x, d, u, w, ei, h = got[:6]
        if rnd == 0:
            sx, mx = got[6:]
    gathered = lax.all_to_all(gap, ("grp", "dom"), 0, 0, tiled=True)
    (v,) = call(final_body, [PLANES], [], [VM] * 6)(
        gathered, schur_inverse, inv_before, pick_t, change, v
    )
    shape = displacement.shape
    return u.reshape(shape), v.reshape(shape)


def solution(mesh):
    return jax.shard_map(
        on_device,
        mesh=mesh,
        in_specs=(
            P("grp", None, "dom", None, None),
            P("grp", None, "dom", None, None),
            P("grp", None, "dom", None, None),
            P("grp", "dom", None, None),
            P("grp", "dom", None, None),
            P("grp", None, None),
            P("grp"),
            P("grp", "dom"),
            P("grp", "dom"),
            P("grp", None, "dom"),
            P(("grp", "dom"), None),
        ),
        out_specs=(P("grp", None, "dom", None, None), P("grp", None, "dom", None, None)),
        check_vma=False,
    )
```

```python
import jax
import jax.numpy as jnp
import numpy as np
from jax import lax
from jax.experimental import pallas as pl
from jax.experimental.pallas import tpu as pltpu
from jax.sharding import PartitionSpec as P


MAXSUB = 8
ROUNDS = MAXSUB // 2
GROUPS = 4
DOMS = 32
COARSE = 0.4
ROWS = 96
HALF = ROWS // 2
COLS = 128
WIDTH = 256
F32 = jnp.float32
BF16 = jnp.bfloat16
VM = pl.BlockSpec(memory_space=pltpu.VMEM)
SM = pl.BlockSpec(memory_space=pltpu.SMEM)
HBM = pl.BlockSpec(memory_space=pltpu.HBM)


def describe():
    return [
        (at, q // 8, q % 8, part == 2) for at in range(3) for part in range(3) for q in range(16)
    ]


def selectors():
    pick_row = np.zeros((2, 32, 24), np.float32)
    pick_col = np.zeros((2, 2, 24, WIDTH), np.float32)
    for w in range(2):
        for be in range(4):
            for q in range(6):
                pick_row[w, be * 8 + q, (4 * (q % 2 ^ w) + be) * 3 + q // 2] = 1.0
        for t in range(2):
            for k, (at, e, q, _) in enumerate(describe()):
                if q < 6 and at - t in (0, 1):
                    pick_col[w, t, (4 * (q % 2 ^ w) + 2 * (at - t) + e) * 3 + q // 2, k] = 1.0
    return pick_row, pick_col


PICK_ROW, PICK_COL = selectors()


def step_size(count_ref):
    count = jnp.full((8, COLS), count_ref[0], jnp.int32).astype(F32)
    return COARSE / count


def lane_up(x):
    return pltpu.roll(x, COLS - 1, 1)


def lane_down(x):
    return pltpu.roll(x, 1, 1)


def every(i, stride=8):
    return pl.ds(i, ROWS, stride=stride)


def tile(r):
    return slice(8 * (r % ROWS), 8 * (r % ROWS) + 8)


def halves(u):
    hi = u.astype(BF16)
    return hi, (u - hi.astype(F32)).astype(BF16)


def tile_rows(get, rotated=None):
    done = {}

    def one(r):
        r %= ROWS
        if r not in done:
            here = get(r)
            shifted = lane_up(here) if rotated is None else rotated(r)
            done[r] = halves(jnp.concatenate([here, shifted], 0))
        hi, lo = done[r]
        return [hi, lo, hi]

    def rows(r):
        pad = jnp.zeros((WIDTH - 144, COLS), BF16)
        return jnp.concatenate(one(r) + one(r + 1) + one(r + 2) + [pad], 0)

    return rows


def sweep(start, terms, finish):
    carry = {}
    first = {}

    def close(r, a, b):
        finish(r, (a[0] + b[0]) + lane_down(a[1] + b[1]))

    for i in range(start, start + HALF, 2):
        outs = []
        for rows, lhs, _ in terms:
            rhs = jnp.concatenate([rows(i), rows(i + HALF)], 1)
            outs.append(jnp.dot(lhs, rhs, preferred_element_type=F32))
        for h in range(2):
            for t in range(2):
                r = i + t + h * HALF
                part = []
                for be in range(4):
                    j = 32 * t + 8 * be
                    block = [
                        scale[tile(r), :] * out[j : j + 8, h * COLS : (h + 1) * COLS]
                        for (_, _, scale), out in zip(terms, outs)
                    ]
                    part.append(sum(block[1:], block[0]))
                if i + t == start:
                    first[h] = part[:2]
                else:
                    close(r, part[:2], carry[h])
                carry[h] = part[2:]
    close(start, first[0], carry[1])
    close(start + HALF, first[1], carry[0])


def weights_of(a_ref, n):
    return a_ref[64 * n : 64 * n + 64, :]


def inner_pass(a_ref, si, e, m, u, w, ei_out, h_out):
    def finish(r, force):
        at = tile(r)
        rest = e[at, :] - m[at, :] * force
        ei_out[at, :] = rest
        h_out[at, :] = u[at, :] + (w[at, :] + rest)

    sweep(2, [(tile_rows(lambda r: u[tile(r), :]), weights_of(a_ref, 0), si)], finish)


def send_edges(u, h, x_msg, d_msg):
    for base, src in ((0, u), (3, h)):
        for c in range(3):
            x_msg[base + c] = src[every(2 * c), :]
            d_msg[base + c] = src[every(2 * c + 1), :]


def blank_pads(*refs):
    zero = jnp.zeros((ROWS, COLS), F32)
    for q in (6, 7):
        for ref in refs:
            ref[every(q), :] = zero


def prep_body(
    count_ref, place_ref, kmat_h, row_h, col_h, u_h, scale_h, v_h, mass_h, ext_h,
    x_msg, d_msg, u_t, w_t, e_t, m_t, ei_t, h_t, si_t, a_out,
    kmat, row, col, u_n, scale, v_n, mass, ext_n, sems,
):
    pairs = [
        (kmat_h, kmat), (row_h, row), (col_h, col), (u_h, u_n),
        (scale_h, scale), (v_h, v_n), (mass_h, mass), (ext_h, ext_n),
    ]
    copies = [pltpu.make_async_copy(a, b, sems.at[n]) for n, (a, b) in enumerate(pairs)]
    for copy in copies:
        copy.start()
    blank_pads(u_t, w_t, e_t, m_t, si_t)
    odd = place_ref[0] % 2 == 1
    dt = step_size(count_ref)[0:1]
    high = lax.Precision.HIGHEST
    for copy in copies[:3]:
        copy.wait()
    slot = lax.broadcasted_iota(jnp.int32, (64, WIDTH), 1)
    low = slot % 48 >= 32
    full = []
    for layer in range(2):
        flip = odd if layer == 0 else jnp.logical_not(odd)
        rows = jnp.dot(
            jnp.where(flip, row[1], row[0]), kmat[...], precision=high, preferred_element_type=F32
        )
        cols = [jnp.where(flip, col[1, t], col[0, t]) for t in range(2)]
        blocks = [jnp.dot(rows, c, precision=high, preferred_element_type=F32) for c in cols]
        block = jnp.concatenate(blocks, 0)
        big = block.astype(BF16).astype(F32)
        full.append(jnp.where(low, block - big, big).astype(BF16))
    across = (lax.broadcasted_iota(jnp.int32, (64, WIDTH), 0) % 2) == 0
    a_out[0:64, :] = full[0]
    a_out[64:128, :] = full[1]
    a_out[128:192, :] = jnp.where(across, full[1].astype(F32), 0.0).astype(BF16)
    a_out[192:256, :] = jnp.where(across, 0.0, full[1].astype(F32)).astype(BF16)

    def sides(ref, k=None):
        low_plane, top_plane = (ref[0], ref[1]) if k is None else (ref[2 * k], ref[2 * k + 1])
        return jnp.where(odd, top_plane, low_plane), jnp.where(odd, low_plane, top_plane)

    for copy in copies[3:]:
        copy.wait()
    inv = [(dt * dt) / part for part in sides(mass)]
    for c in range(3):
        us, vs, es = sides(u_n, c), sides(v_n, c), sides(ext_n, c)
        for x in range(2):
            at = every(2 * c + x)
            u_t[at, :] = us[x]
            w_t[at, :] = dt * vs[x]
            e_t[at, :] = inv[x] * es[x]
            m_t[at, :] = inv[x]
            si_t[at, :] = scale[0]
    inner_pass(a_out, si_t, e_t, m_t, u_t, w_t, ei_t, h_t)
    send_edges(u_t, h_t, x_msg, d_msg)
    x_msg[6] = inv[0]
    d_msg[6] = inv[1]
    x_msg[7] = scale[1]
    d_msg[7] = scale[1]


def taken(x):
    sub = lax.broadcasted_iota(jnp.int32, (8, COLS), 0)
    return (sub % 2 == x) & (sub < 6)


def outer_step(rnd, x, planes, scale, count_ref, refs):
    u_t, w_t, m_t, ei_t, h_t, a_ref, s_t, mm_t, ur, hr, u1, w1 = refs
    act = jnp.where(count_ref[0] > 2 * rnd, 1.0, 0.0).astype(F32)
    mask = taken(1 - x)
    for c in range(3):
        at = every(2 * c + 1 - x)
        ur[at, :] = planes(c)
        hr[at, :] = planes(3 + c)
        if rnd == 0:
            mm_t[at, :] = planes(6)
    if rnd == 0:
        blank_pads(s_t)
        for q in range(6):
            s_t[every(q), :] = scale
        for r in range(ROWS):
            mm_t[tile(r), :] = jnp.where(mask, mm_t[tile(r), :], m_t[tile(r), :])

    def get(r):
        return jnp.where(mask, ur[tile(r), :], u_t[tile(r), :])

    def finish(r, force):
        at = tile(r)
        pull = mm_t[at, :] * force
        u = get(r)
        goal = jnp.where(mask, hr[at, :], h_t[at, :])
        u1[at, :] = u + act * ((goal - pull) - u)
        w1[at, :] = w_t[at, :] + act * (ei_t[at, :] - pull)

    sweep(0, [(tile_rows(get), weights_of(a_ref, 1), s_t)], finish)


def within_body(rnd, *refs):
    refs = list(refs)
    take = lambda n: [refs.pop(0) for _ in range(n)]
    count_ref, place_ref, d_in, u_t, w_t, m_t, ei_t, h_t, a_ref = take(9)
    (scale,) = take(1) if rnd == 0 else (None,)
    if rnd > 0:
        sd_t, md_t = take(2)
    u1, w1, fd, u1_shift = take(4)
    if rnd == 0:
        sd_t, md_t = take(2)
    ur, hr = take(2)
    odd = place_ref[0] % 2 == 1
    layer = jnp.where(odd, d_in[7], scale[1]) if rnd == 0 else None
    outer_step(
        rnd, 1, lambda k: d_in[k], layer, count_ref,
        (u_t, w_t, m_t, ei_t, h_t, a_ref, sd_t, md_t, ur, hr, u1, w1),
    )

    def finish(r, force):
        fd[tile(r), :] = force

    def rotated(r):
        u1_shift[tile(r), :] = lane_up(u1[tile(r), :])
        return u1_shift[tile(r), :]

    rows = tile_rows(lambda r: u1[tile(r), :], rotated)
    sweep(1, [(rows, weights_of(a_ref, 3), sd_t)], finish)


def across_body(rnd, *refs):
    refs = list(refs)
    take = lambda n: [refs.pop(0) for _ in range(n)]
    last = rnd == ROUNDS - 1
    count_ref, place_ref, x_in, u_t, w_t, e_t, m_t, ei_t, h_t, si_t, a_ref, u1d, w1d, fd, u1d_shift = take(15)
    (scale,) = take(1) if rnd == 0 else (None,)
    if rnd > 0:
        sx_t, mx_t = take(2)
    if last:
        pick, share = take(2)
        u_out, v_out, g_out = take(3)
    else:
        x_msg, d_msg, u2, w2, ei_out, h_out = take(6)
    if rnd == 0:
        sx_t, mx_t = take(2)
    ur, hr, u1x, w1x, _ = take(5)
    if last:
        u2, w2 = take(2)
    place = place_ref[0]
    odd = place % 2 == 1
    inside = (place > 0) & (place < DOMS - 1)

    def planes(k):
        return jnp.where(inside, x_in[k], 0.0)

    layer = jnp.where(odd, scale[1], planes(7)) if rnd == 0 else None
    outer_step(
        rnd, 0, planes, layer, count_ref,
        (u_t, w_t, m_t, ei_t, h_t, a_ref, sx_t, mx_t, ur, hr, u1x, w1x),
    )
    act = jnp.where(count_ref[0] > 2 * rnd + 1, 1.0, 0.0).astype(F32)
    within = lax.broadcasted_iota(jnp.int32, (8, COLS), 0) % 2 == 1

    def middle(r):
        return jnp.where(within, u1d[tile(r), :], u1x[tile(r), :])

    def finish(r, force):
        at = tile(r)
        w = jnp.where(within, w1d[at, :], w1x[at, :])
        w = w + act * (e_t[at, :] - m_t[at, :] * (force + fd[at, :]))
        w2[at, :] = w
        u2[at, :] = middle(r) + act * w

    shifts = {}

    def shift_x(r):
        if r not in shifts:
            shifts[r] = lane_up(u1x[tile(r), :])
        return shifts[r]

    def shift_middle(r):
        return jnp.where(within, u1d_shift[tile(r), :], shift_x(r))

    sweep(
        1,
        [
            (tile_rows(middle, shift_middle), weights_of(a_ref, 0), si_t),
            (tile_rows(lambda r: u1x[tile(r), :], shift_x), weights_of(a_ref, 2), sx_t),
        ],
        finish,
    )
    if last:
        back = 1.0 / step_size(count_ref)[0:1]
        for src, out, scaled in ((w2, v_out, True), (u2, u_out, False)):
            for c in range(3):
                here, there = src[every(2 * c), :], src[every(2 * c + 1), :]
                if scaled:
                    here, there = here * back, there * back
                out[2 * c] = jnp.where(odd, there, here)
                out[2 * c + 1] = jnp.where(odd, here, there)
        partial_gaps(place_ref, pick, share, v_out, g_out)
        return
    inner_pass(a_ref, si_t, e_t, m_t, u2, w2, ei_out, h_out)
    send_edges(u2, h_out, x_msg, d_msg)


def thirds(x):
    parts = []
    for _ in range(3):
        part = x.astype(jnp.bfloat16)
        parts.append(part)
        x = x - part.astype(F32)
    return parts


def chosen(onehot, values):
    return sum(jnp.dot(onehot, part, preferred_element_type=F32) for part in thirds(values))


def node_body(own, peer, normal, before, mass, pick, pick_t, share, change):
    sub = lax.broadcasted_iota(jnp.int32, (16, 16), 0)
    eye = sub == lax.broadcasted_iota(jnp.int32, (16, 16), 1)
    lane = lax.broadcasted_iota(jnp.int32, (16, COLS), 1)
    weights = jnp.concatenate([mass[0], mass[1]], 1)

    def column(line):
        return jnp.sum(jnp.where(eye, jnp.broadcast_to(line, (16, 16)), 0.0), axis=1, keepdims=True)

    for side, nodes, vec, sign in ((0, own, normal, 1.0), (1, peer, before, -1.0)):
        at = slice(16 * side, 16 * side + 16)
        index = column(nodes[...].astype(F32)).astype(jnp.int32)
        plane = jnp.where(index >= ROWS * COLS, 1, 0)
        rest = index - plane * (ROWS * COLS)
        row = rest // COLS
        col = rest - row * COLS
        onehot = jnp.where(lane == row, 1.0, 0.0)
        pick[at, :] = onehot[:, 0:ROWS].astype(jnp.bfloat16)
        heavy = chosen(onehot[:, 0:ROWS].astype(jnp.bfloat16), weights)
        hits = [(lane == col) & (plane == p) for p in range(2)]
        total = jnp.where(hits[0], heavy[:, 0:COLS], 0.0) + jnp.where(hits[1], heavy[:, COLS:], 0.0)
        total = jnp.sum(total, axis=1, keepdims=True)
        for c in range(3):
            value = sign * column(vec[c : c + 1, :])
            for p in range(2):
                q = 2 * c + p
                part = jnp.where(hits[p], value, 0.0)
                share[at, q * COLS : (q + 1) * COLS] = part
                change[at, q * COLS : (q + 1) * COLS] = -part / total
        pick_t[side] = jnp.transpose(onehot)[0:ROWS].astype(jnp.bfloat16)


def partial_gaps(place_ref, pick, share, v, g_out):
    values = jnp.concatenate([v[q] for q in range(6)], 1)
    total = jnp.sum(chosen(pick[...], values) * share[...], axis=1, keepdims=True)
    lane = lax.broadcasted_iota(jnp.int32, (32, COLS), 1)
    sub = lax.broadcasted_iota(jnp.int32, (32, COLS), 0)
    line = jnp.where(lane == sub % 16 + 16 * (place_ref[0] % 8), jnp.broadcast_to(total, (32, COLS)), 0.0)
    for side in range(2):
        part = jnp.sum(line[16 * side : 16 * side + 16], axis=0, keepdims=True)
        g_out[:, side * COLS : (side + 1) * COLS] = jnp.broadcast_to(part, (128, COLS))


def final_body(gathered, inv_own, inv_before, pick_t, change, u_in, v_in, u_out, v_out, plane, sems):
    copies = [pltpu.make_async_copy(u_in, u_out, sems.at[6])]
    copies[0].start()
    mine = jnp.sum(gathered[:, 0:COLS].reshape(16, 8, COLS), axis=1)
    other = jnp.sum(gathered[:, COLS : 2 * COLS].reshape(16, 8, COLS), axis=1)
    gap = mine + jnp.concatenate([other[4:16], other[0:4]], 0)
    total = None
    for side, rows in ((0, inv_own), (1, inv_before)):
        acc = jnp.zeros((16, COLS), F32)
        for k in range(16):
            acc = acc + rows[:, k * COLS : (k + 1) * COLS] * gap[k : k + 1, :]
        lam = jnp.sum(acc, axis=1, keepdims=True)
        part = chosen(pick_t[side], change[16 * side : 16 * side + 16, :] * lam)
        total = part if total is None else total + part
    for q in range(6):
        plane[q] = v_in[q] + total[:, q * COLS : (q + 1) * COLS]
        copies.append(pltpu.make_async_copy(plane.at[q], v_out.at[q], sems.at[q]))
        copies[-1].start()
    for copy in copies:
        copy.wait()


def call(body, outs, scratch, ins, limit=24 * 1024 * 1024, far_outs=()):
    return pl.pallas_call(
        body,
        out_shape=[s if isinstance(s, jax.ShapeDtypeStruct) else jax.ShapeDtypeStruct(s, F32) for s in outs],
        in_specs=ins,
        out_specs=[HBM if n in far_outs else VM for n in range(len(outs))],
        scratch_shapes=[pltpu.VMEM(s, F32) if isinstance(s, tuple) else s for s in scratch],
        compiler_params=pltpu.CompilerParams(vmem_limit_bytes=limit),
    )


TILE = (ROWS * 8, COLS)
PLANES = (6, ROWS, COLS)


def across_pairs():
    pairs = [(g * DOMS + i, g * DOMS + i + 1) for g in range(GROUPS) for i in range(1, DOMS - 1, 2)]
    for g in range(0, GROUPS, 2):
        for i in (0, DOMS - 1):
            pairs.append((g * DOMS + i, (g + 1) * DOMS + i))
    return pairs + [(b, a) for a, b in pairs]


ACROSS = across_pairs()
WITHIN = [(i, i ^ 1) for i in range(DOMS)]
FROM_BEFORE = [(i, (i + 1) % GROUPS) for i in range(GROUPS)]


def far(x):
    return pltpu.with_memory_space_constraint(jnp.asarray(x), pltpu.HBM)


def on_device(
    displacement, velocity, external, mass, elem_scale, stiffness, substeps,
    own_nodes, peer_nodes, normals, schur_inverse,
):
    field = displacement[0].reshape(PLANES)
    speed = velocity[0].reshape(PLANES)
    loads = external[0].reshape(PLANES)
    weight = mass[0]
    scale = elem_scale[0]
    place = lax.axis_index("dom").reshape(1)
    normal = normals[0]
    scalars = (substeps, place)
    b16 = lambda *shape: jax.ShapeDtypeStruct(shape, BF16)

    first = (8, ROWS, COLS)
    pair = (2, ROWS, COLS)
    x, d, u, w, e, m, ei, h, si, a = call(
        prep_body,
        [first, first] + [TILE] * 7 + [b16(256, WIDTH)],
        [
            (24, 24), (2, 32, 24), (2, 2, 24, WIDTH), PLANES, pair, PLANES, pair, PLANES,
            pltpu.SemaphoreType.DMA((8,)),
        ],
        [SM] * 2 + [HBM] * 8,
    )(*scalars, *(far(v) for v in (stiffness[0], PICK_ROW, PICK_COL, field, scale, speed, weight, loads)))
    for rnd in range(ROUNDS):
        last = rnd == ROUNDS - 1
        x = lax.ppermute(x, ("grp", "dom"), ACROSS)
        d = lax.ppermute(d, "dom", WITHIN)
        if rnd == 0:
            inv_before = lax.ppermute(schur_inverse, "grp", FROM_BEFORE)
            before = lax.ppermute(normal, "grp", FROM_BEFORE)

        if rnd == 1:
            nodes = call(
                node_body, [b16(32, ROWS), b16(2, ROWS, 16), (32, 6 * COLS), (32, 6 * COLS)], [], [VM] * 5
            )(own_nodes, peer_nodes, normal, before, weight)
            d, *nodes = lax.optimization_barrier((d, *nodes))
            pick, pick_t, share, change = nodes

        def within(*refs, rnd=rnd):
            return within_body(rnd, *refs)

        args = [d, u, w, m, ei, h, a] + ([scale] if rnd == 0 else [sd, md])
        got = call(
            within, [TILE] * (6 if rnd == 0 else 4), [TILE] * 2, [SM] * 2 + [VM] * len(args)
        )(*scalars, *args)
        u1d, w1d, fd, u1d_shift = got[:4]
        if rnd == 0:
            sd, md = got[4:]
            u1d, inv_before, before = lax.optimization_barrier((u1d, inv_before, before))

        def across(*refs, rnd=rnd):
            return across_body(rnd, *refs)

        args = [x, u, w, e, m, ei, h, si, a, u1d, w1d, fd, u1d_shift] + ([scale] if rnd == 0 else [sx, mx])
        args += [pick, share] if last else []
        outs = [PLANES, PLANES, (128, 2 * COLS)] if last else [PLANES, PLANES] + [TILE] * 4
        outs += [TILE, TILE] if rnd == 0 else []
        scratch = [TILE] * 5 + ([TILE, TILE] if last else [])
        got = call(across, outs, scratch, [SM] * 2 + [VM] * len(args))(*scalars, *args)
        if last:
            u, v, gap = got
        else:
            x, d, u, w, ei, h = got[:6]
        if rnd == 0:
            sx, mx = got[6:]
    gathered = lax.all_to_all(gap, ("grp", "dom"), 0, 0, tiled=True)
    u, v = call(
        final_body, [PLANES, PLANES], [PLANES, pltpu.SemaphoreType.DMA((7,))], [VM] * 7, far_outs=(0, 1)
    )(gathered, schur_inverse, inv_before, pick_t, change, u, v)
    shape = displacement.shape
    return u.reshape(shape), v.reshape(shape)


def solution(mesh):
    return jax.shard_map(
        on_device,
        mesh=mesh,
        in_specs=(
            P("grp", None, "dom", None, None),
            P("grp", None, "dom", None, None),
            P("grp", None, "dom", None, None),
            P("grp", "dom", None, None),
            P("grp", "dom", None, None),
            P("grp", None, None),
            P("grp"),
            P("grp", "dom"),
            P("grp", "dom"),
            P("grp", None, "dom"),
            P(("grp", "dom"), None),
        ),
        out_specs=(P("grp", None, "dom", None, None), P("grp", None, "dom", None, None)),
        check_vma=False,
    )
```
